32 devices in a mesh: dp: 4 (over y, z), sp: 8 (over x, core).
Axes of the slice: x: 4, y: 2, z: 2, core: 2. Of those that a mesh axis runs over, the one named last changes fastest.
The devices are a block of a 4x4x8 slice.
Arguments:
- tok_in: bfloat16 [8192, 7168], P(('dp', 'sp')), parts along dimension 0
- tok_pos: int32 [8192], P(('dp', 'sp')), parts along dimension 0
- w_dq: bfloat16 [7168, 1536], replicated
- g_q: float32 [1536], replicated
- w_uq: bfloat16 [1536, 128, 192], replicated
- w_dkv: bfloat16 [7168, 576], replicated
- g_kv: float32 [512], replicated
- w_uk: bfloat16 [512, 128, 128], replicated
- w_uv: bfloat16 [512, 128, 128], replicated
- w_o: bfloat16 [128, 128, 7168], replicated
Outputs:
- output 1: bfloat16 [8192, 7168], P(('dp', 'sp')), parts along dimension 0
- output 2: bfloat16 [8192, 512], P(('dp', 'sp')), parts along dimension 0
- output 3: bfloat16 [8192, 64], P(('dp', 'sp')), parts along dimension 0
There are 4 independent parts. The reference program is written for one: setup_inputs(seed, part) draws one part's arguments, and reference() takes and returns one part's arrays. A program takes and returns all parts, laid end to end along the dimension named above; an argument that names none is the same for every part.
All inputs are finite; a program needn't handle non-finite values.
Results may differ from the reference program's by a relative error of at most 0.00551604.
Values are sent between devices in bfloat16 or wider.
A program may use at most 768 MiB of HBM per device.

```python
import math
import jax
import jax.numpy as jnp
from jax import lax

SEQ_LEN = 2048
ROW_BLOCK = 256
MODEL_DIM = 7168
NUM_HEADS = 128
Q_RANK = 1536
KV_RANK = 512
NOPE_DIM = 128
ROPE_DIM = 64
V_DIM = 128

ROPE_THETA = 10000.0
YARN_FACTOR = 40.0
ORIG_CTX = 4096.0
BETA_FAST = 32.0
BETA_SLOW = 1.0
NORM_EPS = 1e-6


def rope_freqs(rot_dim):
    half_dim = rot_dim // 2
    log_base = 2.0 * math.log(ROPE_THETA)
    low_idx = max(math.floor(rot_dim * math.log(ORIG_CTX / (BETA_FAST * 2.0 * math.pi)) / log_base), 0)
    high_idx = min(math.ceil(rot_dim * math.log(ORIG_CTX / (BETA_SLOW * 2.0 * math.pi)) / log_base), half_dim - 1)
    spread = max(high_idx - low_idx, 0.001)
    freq_list = []
    for freq_idx in range(half_dim):
        base_freq = ROPE_THETA ** (-2.0 * freq_idx / rot_dim)
        ramp_val = min(max((freq_idx - low_idx) / spread, 0.0), 1.0)
        freq_list.append(base_freq / YARN_FACTOR * ramp_val + base_freq * (1.0 - ramp_val))
    return jnp.asarray(freq_list, dtype=jnp.float32)


def rotate_half(act_in, cos_t, sin_t):
    half_dim = act_in.shape[-1] // 2
    first = act_in[..., :half_dim]
    second = act_in[..., half_dim:]
    return jnp.concatenate([first * cos_t - second * sin_t, second * cos_t + first * sin_t], axis=-1)


def rms_norm(act_in, gain):
    mean_sq = jnp.mean(act_in * act_in, axis=-1, keepdims=True)
    return act_in * lax.rsqrt(mean_sq + NORM_EPS) * gain


def setup_inputs(seed: int = 0, part: int = 0) -> dict:
    root_key = jax.random.key(seed)
    part_key = jax.random.fold_in(root_key, part)
    key_x, key_pos = jax.random.split(part_key)
    weight_keys = jax.random.split(root_key, 8)

    def draw_weight(sub_key, arr_shape, fan_in):
        return (jax.random.normal(sub_key, arr_shape, jnp.float32) * fan_in ** -0.5).astype(jnp.bfloat16)

    tok_in = jax.random.normal(key_x, (SEQ_LEN, MODEL_DIM), jnp.float32).astype(jnp.bfloat16)
    pos_steps = jax.random.randint(key_pos, (SEQ_LEN,), 1, 5, dtype=jnp.int32)
    tok_pos = (jnp.cumsum(pos_steps) - pos_steps[0]).astype(jnp.int32)
    w_dq = draw_weight(weight_keys[0], (MODEL_DIM, Q_RANK), MODEL_DIM)
    g_q = jax.random.uniform(weight_keys[1], (Q_RANK,), jnp.float32, 0.5, 1.5)
    w_uq = draw_weight(weight_keys[2], (Q_RANK, NUM_HEADS, NOPE_DIM + ROPE_DIM), Q_RANK)
    w_dkv = draw_weight(weight_keys[3], (MODEL_DIM, KV_RANK + ROPE_DIM), MODEL_DIM)
    g_kv = jax.random.uniform(weight_keys[4], (KV_RANK,), jnp.float32, 0.5, 1.5)
    w_uk = draw_weight(weight_keys[5], (KV_RANK, NUM_HEADS, NOPE_DIM), KV_RANK)
    w_uv = draw_weight(weight_keys[6], (KV_RANK, NUM_HEADS, V_DIM), KV_RANK)
    w_o = draw_weight(weight_keys[7], (NUM_HEADS, V_DIM, MODEL_DIM), NUM_HEADS * V_DIM)
    return dict(tok_in=tok_in, tok_pos=tok_pos, w_dq=w_dq, g_q=g_q, w_uq=w_uq, w_dkv=w_dkv, g_kv=g_kv, w_uk=w_uk, w_uv=w_uv, w_o=w_o)


def reference(tok_in, tok_pos, w_dq, g_q, w_uq, w_dkv, g_kv, w_uk, w_uv, w_o):
    qk_dim = NOPE_DIM + ROPE_DIM
    attn_scale = (0.1 * math.log(YARN_FACTOR) + 1.0) ** 2 / math.sqrt(qk_dim)
    angles = tok_pos.astype(jnp.float32)[:, None] * rope_freqs(ROPE_DIM)[None, :]
    cos_t = jnp.cos(angles)
    sin_t = jnp.sin(angles)
    q_lat = rms_norm(jnp.dot(tok_in, w_dq, preferred_element_type=jnp.float32), g_q).astype(jnp.bfloat16)
    q_full = jnp.dot(q_lat, w_uq.reshape(Q_RANK, NUM_HEADS * qk_dim), preferred_element_type=jnp.float32).reshape(SEQ_LEN, NUM_HEADS, qk_dim)
    q_nope = q_full[:, :, :NOPE_DIM].astype(jnp.bfloat16)
    q_rot = rotate_half(q_full[:, :, NOPE_DIM:], cos_t[:, None, :], sin_t[:, None, :]).astype(jnp.bfloat16)
    kv_lat = jnp.dot(tok_in, w_dkv, preferred_element_type=jnp.float32)
    cache_kv = rms_norm(kv_lat[:, :KV_RANK], g_kv).astype(jnp.bfloat16)
    cache_pe = rotate_half(kv_lat[:, KV_RANK:], cos_t, sin_t).astype(jnp.bfloat16)
    k_nope = jnp.dot(cache_kv, w_uk.reshape(KV_RANK, NUM_HEADS * NOPE_DIM), preferred_element_type=jnp.float32).reshape(SEQ_LEN, NUM_HEADS, NOPE_DIM).astype(jnp.bfloat16)
    values = jnp.dot(cache_kv, w_uv.reshape(KV_RANK, NUM_HEADS * V_DIM), preferred_element_type=jnp.float32).reshape(SEQ_LEN, NUM_HEADS, V_DIM).astype(jnp.bfloat16)
    key_idx = jnp.arange(SEQ_LEN)
    num_blocks = SEQ_LEN // ROW_BLOCK

    def head_attention(head_in):
        qn_head, qr_head, kn_head, v_head = head_in

        def block_attention(blk_idx):
            start = blk_idx * ROW_BLOCK
            qn_blk = lax.dynamic_slice_in_dim(qn_head, start, ROW_BLOCK, axis=0)
            qr_blk = lax.dynamic_slice_in_dim(qr_head, start, ROW_BLOCK, axis=0)
            logits = jnp.dot(qn_blk, kn_head.T, preferred_element_type=jnp.float32) + jnp.dot(qr_blk, cache_pe.T, preferred_element_type=jnp.float32)
            logits = logits * attn_scale
            row_idx = start + jnp.arange(ROW_BLOCK)
            logits = jnp.where(key_idx[None, :] <= row_idx[:, None], logits, -jnp.inf)
            attn_prob = jax.nn.softmax(logits, axis=-1).astype(jnp.bfloat16)
            return jnp.dot(attn_prob, v_head, preferred_element_type=jnp.float32).astype(jnp.bfloat16)

        return lax.map(block_attention, jnp.arange(num_blocks)).reshape(SEQ_LEN, V_DIM)

    head_outs = lax.map(head_attention, (jnp.swapaxes(q_nope, 0, 1), jnp.swapaxes(q_rot, 0, 1), jnp.swapaxes(k_nope, 0, 1), jnp.swapaxes(values, 0, 1)))
    attn_cat = jnp.swapaxes(head_outs, 0, 1).reshape(SEQ_LEN, NUM_HEADS * V_DIM)
    attn_out = jnp.dot(attn_cat, w_o.reshape(NUM_HEADS * V_DIM, MODEL_DIM), preferred_element_type=jnp.float32).astype(jnp.bfloat16)
    return attn_out, cache_kv, cache_pe
```

```python
import functools
import math
import jax
import jax.numpy as jnp
from jax import lax
from jax.experimental import pallas as pl
from jax.experimental.pallas import tpu as pltpu
from jax.sharding import PartitionSpec as P

ROPE_THETA = 10000.0
YARN_FACTOR = 40.0
ORIG_CTX = 4096.0
BETA_FAST = 32.0
BETA_SLOW = 1.0
NORM_EPS = 1e-6
MESH = pl.DeviceIdType.MESH
LANES = 128
NEG = -1e30
GROUP = 4


def rope_freqs(rot_dim):
    half_dim = rot_dim // 2
    log_base = 2.0 * math.log(ROPE_THETA)
    low_idx = max(math.floor(rot_dim * math.log(ORIG_CTX / (BETA_FAST * 2.0 * math.pi)) / log_base), 0)
    high_idx = min(math.ceil(rot_dim * math.log(ORIG_CTX / (BETA_SLOW * 2.0 * math.pi)) / log_base), half_dim - 1)
    spread = max(high_idx - low_idx, 0.001)
    freq_list = []
    for freq_idx in range(half_dim):
        base_freq = ROPE_THETA ** (-2.0 * freq_idx / rot_dim)
        ramp_val = min(max((freq_idx - low_idx) / spread, 0.0), 1.0)
        freq_list.append(base_freq / YARN_FACTOR * ramp_val + base_freq * (1.0 - ramp_val))
    return jnp.asarray(freq_list, dtype=jnp.float32)


def rotate_half(act_in, cos_t, sin_t):
    half_dim = act_in.shape[-1] // 2
    first = act_in[..., :half_dim]
    second = act_in[..., half_dim:]
    return jnp.concatenate([first * cos_t - second * sin_t, second * cos_t + first * sin_t], axis=-1)


def rms_norm(act_in, gain):
    mean_sq = jnp.mean(act_in * act_in, axis=-1, keepdims=True)
    return act_in * lax.rsqrt(mean_sq + NORM_EPS) * gain


def dot_nt(a, b):
    return lax.dot_general(a, b, (((1,), (1,)), ((), ())), preferred_element_type=jnp.float32)


def dot_nn(a, b):
    return jnp.dot(a, b, preferred_element_type=jnp.float32)


SUB = 16
CBLK = 64


def gather_kernel(n, heads, nope, kv_ref, cq_ref, wt_ref, sel_ref, kv_all, cq_all, wn_ref, wr_ref, tn, tr, send_sem, recv_sem, loc_sem):
    step = pl.program_id(0)
    last = pl.num_programs(0) - 1
    me = lax.axis_index("sp")
    right = lax.rem(me + 2, n)
    left = lax.rem(me + n - 2, n)
    mate = me + 1 - 2 * lax.rem(me, 2)
    rows = kv_ref.shape[0]
    half = rows // 2
    srcs = (kv_ref, cq_ref)
    alls = (kv_all, cq_all)

    def piece(arr, owner, off, size):
        return alls[arr].at[pl.ds(pl.multiple_of(owner * rows + off, half), size)]

    def rcopy(arr, idx, src, owner, off, size, dev):
        return pltpu.make_async_remote_copy(
            src_ref=src, dst_ref=piece(arr, owner, off, size),
            send_sem=send_sem.at[arr, idx], recv_sem=recv_sem.at[arr, idx],
            device_id={"sp": dev}, device_id_type=MESH)

    def copies(arr):
        own = srcs[arr]
        opp = lax.rem(me + 4, n)
        c = {}
        c[0] = rcopy(arr, 0, own.at[pl.ds(0, half)], me, 0, half, right)
        c[1] = rcopy(arr, 1, own.at[pl.ds(half, half)], me, half, half, right)
        c[2] = rcopy(arr, 2, own.at[pl.ds(half, half)], me, half, half, left)
        c[3] = rcopy(arr, 3, own.at[pl.ds(0, half)], me, 0, half, left)
        c[4] = rcopy(arr, 4, own, me, 0, rows, mate)
        c[5] = rcopy(arr, 5, piece(arr, left, 0, half), left, 0, half, right)
        c[6] = rcopy(arr, 6, piece(arr, right, half, half), right, half, half, left)
        c[7] = rcopy(arr, 7, piece(arr, left, 0, rows), left, 0, rows, mate)
        c[8] = rcopy(arr, 8, piece(arr, right, 0, rows), right, 0, rows, mate)
        c[9] = rcopy(arr, 9, piece(arr, opp, 0, half), opp, 0, half, mate)
        c[10] = rcopy(arr, 10, piece(arr, opp, half, half), opp, half, half, mate)
        return c

    ckv = copies(0)
    ccq = copies(1)

    def local(arr):
        return pltpu.make_async_copy(srcs[arr], piece(arr, me, 0, rows), loc_sem.at[arr])

    @pl.when(step == 0)
    def _():
        barrier = pltpu.get_barrier_semaphore()
        for dev in (left, right, mate):
            pl.semaphore_signal(barrier, inc=1, device_id={"sp": dev}, device_id_type=MESH)
        pl.semaphore_wait(barrier, 3)
        for c in (ckv, ccq):
            for i in (0, 2, 1, 3, 4):
                c[i].start()
        for arr in range(2):
            local(arr).start()

    @pl.when(step == last // 4)
    def _():
        ckv[0].wait_recv()
        ckv[5].start()
        ckv[2].wait_recv()
        ckv[6].start()

    @pl.when(step == last // 2)
    def _():
        ckv[1].wait_recv()
        ckv[7].start()
        ckv[3].wait_recv()
        ckv[8].start()

    @pl.when(step == (3 * last) // 4)
    def _():
        ccq[0].wait_recv()
        ccq[5].start()
        ccq[2].wait_recv()
        ccq[6].start()

    for s in range(CBLK // SUB):
        lhs = jnp.concatenate([wt_ref[s * SUB + i] for i in range(SUB)], axis=1)
        g = dot_nn(lhs, sel_ref[...])
        width = g.shape[1] // 2
        tn[s] = g[:nope].T
        tr[s] = jnp.concatenate([g[nope:, :width], g[nope:, width:]], axis=0).T
        pairs = heads // 2
        for h in range(heads):
            par, hp = h % 2, h // 2
            wn_ref[s * SUB:(s + 1) * SUB, h * nope:(h + 1) * nope] = tn[s, pl.ds(par * width + hp, SUB, stride=pairs), :].astype(jnp.bfloat16)
        for hp in range(pairs):
            wr_ref[s * SUB:(s + 1) * SUB, hp * LANES:(hp + 1) * LANES] = tr[s, pl.ds(hp, SUB, stride=pairs), :].astype(jnp.bfloat16)

    @pl.when(step == last)
    def _():
        ccq[1].wait_recv()
        ccq[7].start()
        ccq[3].wait_recv()
        ccq[8].start()
        for c in (ckv, ccq):
            c[5].wait_recv()
            c[9].start()
            c[6].wait_recv()
            c[10].start()
        for c in (ckv, ccq):
            for i in (4, 7, 8, 9, 10):
                c[i].wait_recv()
            for i in range(11):
                c[i].wait_send()
        for arr in range(2):
            local(arr).wait()


def gather_and_pick(n, heads, nope, kv_own, cq_own, w_t, sel):
    rows, kvw = kv_own.shape
    rank = cq_own.shape[1]
    qk = w_t.shape[1]
    bf = jnp.bfloat16
    return pl.pallas_call(
        functools.partial(gather_kernel, n, heads, nope),
        grid=(rank // CBLK,),
        in_specs=[
            pl.BlockSpec((rows, kvw), lambda s: (0, 0)),
            pl.BlockSpec((rows, rank), lambda s: (0, 0)),
            pl.BlockSpec((CBLK, qk, w_t.shape[2]), lambda s: (s, 0, 0)),
            pl.BlockSpec(sel.shape, lambda s: (0, 0)),
        ],
        out_specs=[
            pl.BlockSpec(memory_space=pl.ANY),
            pl.BlockSpec(memory_space=pl.ANY),
            pl.BlockSpec((CBLK, heads * nope), lambda s: (s, 0)),
            pl.BlockSpec((CBLK, heads * (qk - nope)), lambda s: (s, 0)),
        ],
        out_shape=[
            jax.ShapeDtypeStruct((n * rows, kvw), bf),
            jax.ShapeDtypeStruct((n * rows, rank), bf),
            jax.ShapeDtypeStruct((rank, heads * nope), bf),
            jax.ShapeDtypeStruct((rank, heads * (qk - nope)), bf),
        ],
        scratch_shapes=[
            pltpu.VMEM((CBLK // SUB, SUB * heads, nope), jnp.float32),
            pltpu.VMEM((CBLK // SUB, SUB * heads // 2, LANES), jnp.float32),
            pltpu.SemaphoreType.DMA((2, 11)),
            pltpu.SemaphoreType.DMA((2, 11)),
            pltpu.SemaphoreType.DMA((2,)),
        ],
        compiler_params=pltpu.CompilerParams(collective_id=0, has_side_effects=True, dimension_semantics=("arbitrary",)),
        cost_estimate=pl.CostEstimate(flops=30_000_000_000, bytes_accessed=90_000_000, transcendentals=0),
        name="gather_pick",
    )(kv_own, cq_own, w_t, sel)


QB = 512


def attn_kernel(scale2, kv_rank, nope, rot, kv_ref, cq_ref, cos_ref, sin_ref, wn_ref, wr_ref, uk_ref, uvt_ref, o_ref, kcat, vt, qcat, acc, mrow, lrow):
    b = pl.program_id(0)
    vd = uvt_ref.shape[0] // GROUP
    bf = jnp.bfloat16

    @pl.when(b == 0)
    def _():
        def fill(i, _):
            r = pl.ds(pl.multiple_of(i * QB, QB), QB)
            c = kv_ref[r, :kv_rank]
            k = dot_nn(c, uk_ref[...]).astype(bf)
            raw = kv_ref[r, kv_rank:kv_rank + LANES].astype(jnp.float32)
            lane = lax.broadcasted_iota(jnp.int32, raw.shape, 1)
            pe_f = jnp.where(lane < rot, raw, 0.0)
            pe = (pe_f.astype(bf), pltpu.roll(pe_f, rot, 1).astype(bf))
            for h in range(GROUP):
                kcat[h, r, :nope] = k[:, h * nope:(h + 1) * nope]
                kcat[h, r, nope:] = pe[h % 2]
            vt[:, r] = dot_nt(uvt_ref[...], c).astype(bf)
            return 0
        lax.fori_loop(0, kv_ref.shape[0] // QB, fill, 0)

    cq = cq_ref[...]
    qn = dot_nn(cq, wn_ref[...]).astype(bf)
    qr = dot_nn(cq, wr_ref[...])
    cos_t = cos_ref[...]
    sin_t = sin_ref[...]
    for pr in range(GROUP // 2):
        z = qr[:, pr * LANES:(pr + 1) * LANES]
        lane = lax.broadcasted_iota(jnp.int32, z.shape, 1)
        hd = rot // 2
        swapped = jnp.where((lane // hd) % 2 == 0, pltpu.roll(z, LANES - hd, 1), pltpu.roll(z, hd, 1))
        zr = (z * cos_t + swapped * sin_t).astype(bf)
        for m in range(2):
            h = 2 * pr + m
            qcat[h, :, :nope] = qn[:, h * nope:(h + 1) * nope]
            qcat[h, :, nope:] = zr

    hb = QB // 2
    r0 = pl.multiple_of(b * QB, QB)
    tri = lax.broadcasted_iota(jnp.int32, (hb, hb), 0) <= lax.broadcasted_iota(jnp.int32, (hb, hb), 1)
    for h in range(GROUP):
        vrow = slice(h * vd, (h + 1) * vd)
        q0 = qcat[h, :hb, :]
        q1 = qcat[h, hb:, :]
        k0 = kcat[h, pl.ds(r0, hb), :]
        s00 = jnp.where(tri, dot_nt(k0, q0), NEG)
        m0 = jnp.max(s00, axis=0, keepdims=True)
        p00 = jnp.exp2((s00 - m0) * scale2)
        l0 = jnp.sum(p00, axis=0, keepdims=True)
        acc[h, :, :hb] = dot_nn(vt[vrow, pl.ds(r0, hb)], p00.astype(bf))
        k01 = kcat[h, pl.ds(r0, QB), :]
        s1 = dot_nt(k01, q1)
        s10 = s1[:hb]
        s11 = jnp.where(tri, s1[hb:], NEG)
        m1 = jnp.maximum(jnp.max(s10, axis=0, keepdims=True), jnp.max(s11, axis=0, keepdims=True))
        p10 = jnp.exp2((s10 - m1) * scale2)
        p11 = jnp.exp2((s11 - m1) * scale2)
        l1 = jnp.sum(p10, axis=0, keepdims=True) + jnp.sum(p11, axis=0, keepdims=True)
        p1 = jnp.concatenate([p10.astype(bf), p11.astype(bf)], axis=0)
        acc[h, :, hb:] = dot_nn(vt[vrow, pl.ds(r0, QB)], p1)
        mrow[h, :, :hb] = m0
        mrow[h, :, hb:] = m1
        lrow[h, :, :hb] = l0
        lrow[h, :, hb:] = l1

    def body(kb, _):
        r = pl.multiple_of(kb * QB, QB)
        for h in range(GROUP):
            vrow = slice(h * vd, (h + 1) * vd)
            s = dot_nt(kcat[h, pl.ds(r, QB), :], qcat[h])
            m_old = mrow[h]
            m_new = jnp.maximum(m_old, jnp.max(s, axis=0, keepdims=True))
            p = jnp.exp2((s - m_new) * scale2)
            alpha = jnp.exp2((m_old - m_new) * scale2)
            mrow[h] = m_new
            lrow[h] = lrow[h] * alpha + jnp.sum(p, axis=0, keepdims=True)
            acc[h] = acc[h] * alpha + dot_nn(vt[vrow, pl.ds(r, QB)], p.astype(bf))
        return 0

    lax.fori_loop(0, b, body, 0)

    for h in range(GROUP):
        o_ref[:, h * vd:(h + 1) * vd] = (acc[h] / lrow[h]).T.astype(bf)


def attention_group(g, scale2, kv_rank, nope, rot, vd, kv_all, cq_all, cos2, sin2, wn, wr, uk, uvt):
    seq, rank = cq_all.shape
    bf = jnp.bfloat16
    f32 = jnp.float32
    pairs = seq * (seq + QB) // 2
    flops = 2 * GROUP * (seq * rank * (nope + rot) + seq * kv_rank * (nope + vd) + pairs * (nope + rot + vd) * 2)
    return pl.pallas_call(
        functools.partial(attn_kernel, scale2, kv_rank, nope, rot),
        grid=(seq // QB,),
        in_specs=[
            pl.BlockSpec(kv_all.shape, lambda b: (0, 0)),
            pl.BlockSpec((QB, rank), lambda b: (b, 0)),
            pl.BlockSpec((QB, LANES), lambda b: (b, 0)),
            pl.BlockSpec((QB, LANES), lambda b: (b, 0)),
            pl.BlockSpec((rank, GROUP * nope), lambda b: (0, g)),
            pl.BlockSpec((rank, GROUP * rot), lambda b: (0, g)),
            pl.BlockSpec((kv_rank, GROUP * nope), lambda b: (0, g)),
            pl.BlockSpec((GROUP * vd, kv_rank), lambda b: (g, 0)),
        ],
        out_specs=pl.BlockSpec((QB, GROUP * vd), lambda b: (b, 0)),
        out_shape=jax.ShapeDtypeStruct((seq, GROUP * vd), bf),
        scratch_shapes=[
            pltpu.VMEM((GROUP, seq, nope + LANES), bf),
            pltpu.VMEM((GROUP * vd, seq), bf),
            pltpu.VMEM((GROUP, QB, nope + LANES), bf),
            pltpu.VMEM((GROUP, vd, QB), f32),
            pltpu.VMEM((GROUP, 1, QB), f32),
            pltpu.VMEM((GROUP, 1, QB), f32),
        ],
        compiler_params=pltpu.CompilerParams(dimension_semantics=("arbitrary",), vmem_limit_bytes=60_000_000),
        cost_estimate=pl.CostEstimate(flops=flops, bytes_accessed=12_000_000, transcendentals=pairs * GROUP),
        name="mla_attn",
    )(kv_all, cq_all, cos2, sin2, wn, wr, uk, uvt)


def out_kernel(first, final, *refs):
    if first:
        o_ref, w_ref, out_ref = refs[:3]
    else:
        acc_in, o_ref, w_ref, out_ref = refs[:4]
    acc = refs[-1] if final else out_ref
    step = pl.program_id(0)
    hw = w_ref.shape[0] * w_ref.shape[1]
    n = w_ref.shape[2]
    tile = 1024
    for t in range(n // tile):
        cols = slice(t * tile, (t + 1) * tile)
        prod = dot_nn(o_ref[...], w_ref[:, :, cols].reshape(hw, tile))
        if first:
            @pl.when(step == 0)
            def _():
                acc[:, cols] = prod

            @pl.when(step > 0)
            def _():
                acc[:, cols] += prod
        else:
            @pl.when(step == 0)
            def _():
                acc[:, cols] = acc_in[:, cols] + prod

            @pl.when(step > 0)
            def _():
                acc[:, cols] += prod
    if final:
        @pl.when(step == pl.num_programs(0) - 1)
        def _():
            out_ref[...] = acc[...].astype(out_ref.dtype)


def out_product(acc, o, w_o, chunk0, chunks, per_dev, n, final):
    seq, width = o.shape
    rows = seq // n
    hidden = w_o.shape[2]
    hc = width // w_o.shape[1] // chunks
    first = acc is None
    blocks = per_dev // hc
    steps = n * chunks
    in_specs = [] if first else [pl.BlockSpec((rows, hidden), lambda s: (0, 0), pipeline_mode=pl.Buffered(buffer_count=1))]
    in_specs += [
        pl.BlockSpec((rows, hc * w_o.shape[1]), lambda s: (s // chunks, s % chunks)),
        pl.BlockSpec((hc, w_o.shape[1], hidden), lambda s: ((s // chunks) * blocks + chunk0 + s % chunks, 0, 0)),
    ]
    args = ([] if first else [acc]) + [o, w_o]
    return pl.pallas_call(
        functools.partial(out_kernel, first, final),
        grid=(steps,),
        in_specs=in_specs,
        out_specs=pl.BlockSpec((rows, hidden), lambda s: (0, 0)),
        out_shape=jax.ShapeDtypeStruct((rows, hidden), jnp.bfloat16 if final else jnp.float32),
        scratch_shapes=[pltpu.VMEM((rows, hidden), jnp.float32)] if final else [],
        compiler_params=pltpu.CompilerParams(dimension_semantics=("arbitrary",), vmem_limit_bytes=60_000_000),
        cost_estimate=pl.CostEstimate(flops=2 * rows * hidden * width * n, bytes_accessed=2 * hidden * width * n, transcendentals=0),
        name="out_product",
    )(*args)


def solution(mesh):
    n = mesh.shape['sp']
    rows_spec = P(('dp', 'sp'), None)
    tok_spec = P(('dp', 'sp'))
    rep = P()

    def local_step(tok_in, tok_pos, w_dq, g_q, w_uq, w_dkv, g_kv, w_uk, w_uv, w_o):
        bf = jnp.bfloat16
        f32 = jnp.float32
        rows = tok_in.shape[0]
        num_heads = w_uq.shape[1]
        heads = num_heads // n
        qk_dim = w_uq.shape[2]
        kv_rank = g_kv.shape[0]
        rot = w_dkv.shape[1] - kv_rank
        nope = qk_dim - rot
        vd = w_uv.shape[2]
        rank = g_q.shape[0]
        scale2 = (0.1 * math.log(YARN_FACTOR) + 1.0) ** 2 / math.sqrt(qk_dim) / math.log(2.0)
        me = lax.axis_index('sp')

        freqs = rope_freqs(rot)
        angles = tok_pos.astype(f32)[:, None] * freqs[None, :]
        kv_lat = jnp.dot(tok_in, w_dkv, preferred_element_type=f32)
        cache_kv = rms_norm(kv_lat[:, :kv_rank], g_kv).astype(bf)
        cache_pe = rotate_half(kv_lat[:, kv_rank:], jnp.cos(angles), jnp.sin(angles)).astype(bf)
        digits = jnp.stack([tok_pos // LANES, tok_pos % LANES], axis=1).astype(bf)
        kv_own = jnp.concatenate([cache_kv, cache_pe, digits, jnp.zeros((rows, LANES - rot - 2), bf)], axis=1)
        cq_own = rms_norm(jnp.dot(tok_in, w_dq, preferred_element_type=f32), g_q).astype(bf)

        ri = lax.broadcasted_iota(jnp.int32, (SUB * num_heads, SUB * heads), 0)
        ci = lax.broadcasted_iota(jnp.int32, (SUB * num_heads, SUB * heads), 1)
        width = SUB * heads // 2
        want_c = (ci % width) // (heads // 2)
        want_h = me * heads + 2 * (ci % (heads // 2)) + ci // width
        sel = ((ri // num_heads == want_c) & (ri % num_heads == want_h)).astype(bf)

        w_t = jnp.transpose(w_uq, (0, 2, 1))
        kv_all, cq_all, wn, wr = gather_and_pick(n, heads, nope, kv_own, cq_own, w_t, sel)

        uk = lax.dynamic_slice_in_dim(w_uk, me * heads, heads, axis=1).reshape(kv_rank, heads * nope)
        uvt = jnp.transpose(lax.dynamic_slice_in_dim(w_uv, me * heads, heads, axis=1), (1, 2, 0)).reshape(heads * vd, kv_rank)

        digs = kv_all[:, kv_rank + rot:kv_rank + rot + 2].astype(f32)
        ang = (digs[:, :1] * LANES + digs[:, 1:2]) * freqs[None, :]
        cos_a, sin_a = jnp.cos(ang), jnp.sin(ang)
        cos2 = jnp.concatenate([cos_a] * 4, axis=1)
        sin2 = jnp.concatenate([-sin_a, sin_a] * 2, axis=1)

        chunks = heads // GROUP
        o_parts = []
        for g in range(chunks):
            o_g = attention_group(g, scale2, kv_rank, nope, rot, vd, kv_all, cq_all, cos2, sin2, wn, wr, uk, uvt)
            o_parts.append(lax.all_to_all(o_g, 'sp', 0, 0, tiled=True))
        acc = None
        for g in range(chunks):
            acc = out_product(acc, o_parts[g], w_o, g, 1, heads, n, g == chunks - 1)
        return acc, cache_kv, cache_pe

    return jax.shard_map(local_step, mesh=mesh, in_specs=(rows_spec, tok_spec, rep, rep, rep, rep, rep, rep, rep, rep), out_specs=(rows_spec, rows_spec, rows_spec), check_vma=False)
```

```python
import functools
import math
import jax
import jax.numpy as jnp
from jax import lax
from jax.experimental import pallas as pl
from jax.experimental.pallas import tpu as pltpu
from jax.sharding import PartitionSpec as P

ROPE_THETA = 10000.0
YARN_FACTOR = 40.0
ORIG_CTX = 4096.0
BETA_FAST = 32.0
BETA_SLOW = 1.0
NORM_EPS = 1e-6
MESH = pl.DeviceIdType.MESH
LANES = 128
NEG = -1e30
GROUP = 4


def rope_freqs(rot_dim):
    half_dim = rot_dim // 2
    log_base = 2.0 * math.log(ROPE_THETA)
    low_idx = max(math.floor(rot_dim * math.log(ORIG_CTX / (BETA_FAST * 2.0 * math.pi)) / log_base), 0)
    high_idx = min(math.ceil(rot_dim * math.log(ORIG_CTX / (BETA_SLOW * 2.0 * math.pi)) / log_base), half_dim - 1)
    spread = max(high_idx - low_idx, 0.001)
    freq_list = []
    for freq_idx in range(half_dim):
        base_freq = ROPE_THETA ** (-2.0 * freq_idx / rot_dim)
        ramp_val = min(max((freq_idx - low_idx) / spread, 0.0), 1.0)
        freq_list.append(base_freq / YARN_FACTOR * ramp_val + base_freq * (1.0 - ramp_val))
    return jnp.asarray(freq_list, dtype=jnp.float32)


def rotate_half(act_in, cos_t, sin_t):
    half_dim = act_in.shape[-1] // 2
    first = act_in[..., :half_dim]
    second = act_in[..., half_dim:]
    return jnp.concatenate([first * cos_t - second * sin_t, second * cos_t + first * sin_t], axis=-1)


def rms_norm(act_in, gain):
    mean_sq = jnp.mean(act_in * act_in, axis=-1, keepdims=True)
    return act_in * lax.rsqrt(mean_sq + NORM_EPS) * gain


def dot_nt(a, b):
    return lax.dot_general(a, b, (((1,), (1,)), ((), ())), preferred_element_type=jnp.float32)


def dot_nn(a, b):
    return jnp.dot(a, b, preferred_element_type=jnp.float32)


def latent_kernel(kv_rank, x_ref, wq_ref, wkvt_ref, gq_ref, gkv_ref, cos_ref, sin_ref, cq_ref, kv_ref, pe_ref, own_ref, acc_q, acc_kv):
    step = pl.program_id(0)
    bf = jnp.bfloat16

    @pl.when(step == 0)
    def _():
        acc_q[...] = jnp.zeros_like(acc_q)
        acc_kv[...] = jnp.zeros_like(acc_kv)

    acc_q[...] += dot_nn(x_ref[...], wq_ref[...])
    acc_kv[...] += dot_nt(x_ref[...], wkvt_ref[...])

    @pl.when(step == pl.num_programs(0) - 1)
    def _():
        cq_ref[...] = rms_norm(acc_q[...], gq_ref[...]).astype(bf)
        lat = rms_norm(acc_kv[:, :kv_rank], gkv_ref[...]).astype(bf)
        kv_ref[...] = lat
        pe = rotate_half(acc_kv[:, kv_rank:], cos_ref[...], sin_ref[...]).astype(bf)
        pe_ref[...] = pe
        own_ref[:, :kv_rank] = lat
        own_ref[:, kv_rank:] = jnp.concatenate([pe, jnp.zeros((pe.shape[0], LANES - pe.shape[1]), bf)], axis=1)


def latents(x, w_dq, w_dkv, g_q, g_kv, cos_t, sin_t):
    rows, hidden = x.shape
    rank = w_dq.shape[1]
    kvw = w_dkv.shape[1]
    kv_rank = g_kv.shape[0]
    rot = kvw - kv_rank
    half = rot // 2
    kb = 512
    bf = jnp.bfloat16
    const = lambda s: (0, 0)
    return pl.pallas_call(
        functools.partial(latent_kernel, kv_rank),
        grid=(hidden // kb,),
        in_specs=[
            pl.BlockSpec((rows, kb), lambda s: (0, s)),
            pl.BlockSpec((kb, rank), lambda s: (s, 0)),
            pl.BlockSpec((kvw, kb), lambda s: (0, s)),
            pl.BlockSpec((1, rank), const),
            pl.BlockSpec((1, kv_rank), const),
            pl.BlockSpec((rows, half), const),
            pl.BlockSpec((rows, half), const),
        ],
        out_specs=[
            pl.BlockSpec((rows, rank), const),
            pl.BlockSpec((rows, kv_rank), const),
            pl.BlockSpec((rows, rot), const),
            pl.BlockSpec((rows, kv_rank + LANES), const),
        ],
        out_shape=[
            jax.ShapeDtypeStruct((rows, rank), bf),
            jax.ShapeDtypeStruct((rows, kv_rank), bf),
            jax.ShapeDtypeStruct((rows, rot), bf),
            jax.ShapeDtypeStruct((rows, kv_rank + LANES), bf),
        ],
        scratch_shapes=[pltpu.VMEM((rows, rank), jnp.float32), pltpu.VMEM((rows, kvw), jnp.float32)],
        compiler_params=pltpu.CompilerParams(dimension_semantics=("arbitrary",)),
        cost_estimate=pl.CostEstimate(flops=2 * rows * hidden * (rank + kvw), bytes_accessed=2 * hidden * (rank + kvw + rows), transcendentals=0),
        name="latents",
    )(x, w_dq, w_dkv.T, g_q[None, :], g_kv[None, :], cos_t, sin_t)


SUB = 16
CBLK = 96


def gather_kernel(n, heads, nope, kv_ref, cs_ref, cq_ref, wt_ref, uk_ref, uv_ref, kv_all, cs_all, cq_all, wn_ref, wr_ref, uko_ref, uvo_ref, sel, tn, tr, tu, send_sem, recv_sem, loc_sem):
    step = pl.program_id(0)
    last = pl.num_programs(0) - 1
    me = lax.axis_index("sp")
    right = lax.rem(me + 2, n)
    left = lax.rem(me + n - 2, n)
    mate = me + 1 - 2 * lax.rem(me, 2)
    opp = lax.rem(me + 4, n)
    srcs = (kv_ref, cs_ref, cq_ref)
    alls = (kv_all, cs_all, cq_all)
    num = len(srcs)
    bf = jnp.bfloat16

    def piece(arr, owner, part):
        rows = srcs[arr].shape[0]
        half = rows // 2
        off, size = ((0, half), (half, half), (0, rows))[part]
        return alls[arr].at[pl.ds(pl.multiple_of(owner * rows + off, half), size)]

    def own(arr, part):
        half = srcs[arr].shape[0] // 2
        return srcs[arr].at[pl.ds(0, half)] if part == 0 else srcs[arr].at[pl.ds(half, half)] if part == 1 else srcs[arr]

    def rcopy(arr, idx, src, owner, part, dev):
        return pltpu.make_async_remote_copy(
            src_ref=src, dst_ref=piece(arr, owner, part),
            send_sem=send_sem.at[arr, idx], recv_sem=recv_sem.at[arr, idx],
            device_id={"sp": dev}, device_id_type=MESH)

    def copies(arr):
        return [
            rcopy(arr, 0, own(arr, 0), me, 0, right),
            rcopy(arr, 1, own(arr, 1), me, 1, right),
            rcopy(arr, 2, own(arr, 1), me, 1, left),
            rcopy(arr, 3, own(arr, 0), me, 0, left),
            rcopy(arr, 4, own(arr, 2), me, 2, mate),
            rcopy(arr, 5, piece(arr, left, 0), left, 0, right),
            rcopy(arr, 6, piece(arr, right, 1), right, 1, left),
            rcopy(arr, 7, piece(arr, left, 2), left, 2, mate),
            rcopy(arr, 8, piece(arr, right, 2), right, 2, mate),
            rcopy(arr, 9, piece(arr, opp, 0), opp, 0, mate),
            rcopy(arr, 10, piece(arr, opp, 1), opp, 1, mate),
        ]

    cps = [copies(arr) for arr in range(num)]
    loc = [pltpu.make_async_copy(srcs[arr], piece(arr, me, 2), loc_sem.at[arr]) for arr in range(num)]
    width = SUB * heads // 2
    pairs = heads // 2
    lanes = wt_ref.shape[2]

    @pl.when(step == 0)
    def _():
        barrier = pltpu.get_barrier_semaphore()
        for dev in (left, right, mate):
            pl.semaphore_signal(barrier, inc=1, device_id={"sp": dev}, device_id_type=MESH)
        pl.semaphore_wait(barrier, 3)
        for arr in (2, 0, 1):
            for i in (0, 2, 1, 3, 4):
                cps[arr][i].start()
        for arr in range(num):
            loc[arr].start()
        hp = lax.broadcasted_iota(jnp.int32, (lanes, 2 * width), 0)
        col = lax.broadcasted_iota(jnp.int32, (lanes, 2 * width), 1)
        want_h = me * heads + 2 * lax.rem(col, pairs) + col // width
        want_c = lax.rem(col, width) // pairs
        code = jnp.where(hp == want_h, want_c, -1)
        for c in range(SUB):
            sel[c * lanes:(c + 1) * lanes, :] = jnp.where(code == c, 1.0, 0.0).astype(bf)

    @pl.when(step == last // 2)
    def _():
        cps[2][0].wait_recv()
        cps[2][5].start()
        cps[2][2].wait_recv()
        cps[2][6].start()

    for s in range(CBLK // SUB):
        lhs = jnp.concatenate([wt_ref[s * SUB + i] for i in range(SUB)], axis=1)
        g = dot_nn(lhs, sel[...])
        tn[s] = g[:nope].T
        tr[s] = jnp.concatenate([g[nope:, :width], g[nope:, width:]], axis=0).T
        for h in range(heads):
            par, hp = h % 2, h // 2
            wn_ref[s * SUB:(s + 1) * SUB, h * nope:(h + 1) * nope] = tn[s, pl.ds(par * width + hp, SUB, stride=pairs), :].astype(bf)
        for hp in range(pairs):
            wr_ref[s * SUB:(s + 1) * SUB, hp * LANES:(hp + 1) * LANES] = tr[s, pl.ds(hp, SUB, stride=pairs), :].astype(bf)

    cb = uk_ref.shape[0]
    for i, (src, dst) in enumerate(((uk_ref, uko_ref), (uv_ref, uvo_ref))):
        wd = src.shape[2]
        tu[i] = src[...].astype(jnp.float32).reshape(cb * heads, wd)
        for h in range(heads):
            dst[:, h * wd:(h + 1) * wd] = tu[i, pl.ds(h, cb, stride=heads), :].astype(bf)

    @pl.when(step == last)
    def _():
        cps[2][1].wait_recv()
        cps[2][7].start()
        cps[2][3].wait_recv()
        cps[2][8].start()
        for arr in (0, 1):
            cps[arr][0].wait_recv()
            cps[arr][5].start()
            cps[arr][2].wait_recv()
            cps[arr][6].start()
        for arr in (0, 1):
            cps[arr][1].wait_recv()
            cps[arr][7].start()
            cps[arr][3].wait_recv()
            cps[arr][8].start()
        for arr in (2, 0, 1):
            cps[arr][5].wait_recv()
            cps[arr][9].start()
            cps[arr][6].wait_recv()
            cps[arr][10].start()
        for arr in range(num):
            for i in (4, 7, 8, 9, 10):
                cps[arr][i].wait_recv()
            for i in range(11):
                cps[arr][i].wait_send()
            loc[arr].wait()


def gather_and_pick(n, heads, nope, kv_own, cs_own, cq_own, w_t, w_uk, w_uv):
    rank = cq_own.shape[1]
    qk = w_t.shape[1]
    kv_rank = w_uk.shape[0]
    vd = w_uv.shape[2]
    steps = rank // CBLK
    cb = kv_rank // steps
    bf = jnp.bfloat16
    f32 = jnp.float32
    const = lambda s: (0, 0)
    own_heads = lambda s: (s, lax.axis_index("sp"), 0)
    return pl.pallas_call(
        functools.partial(gather_kernel, n, heads, nope),
        grid=(steps,),
        in_specs=[
            pl.BlockSpec(kv_own.shape, const),
            pl.BlockSpec(cs_own.shape, const),
            pl.BlockSpec(cq_own.shape, const),
            pl.BlockSpec((CBLK, qk, w_t.shape[2]), lambda s: (s, 0, 0)),
            pl.BlockSpec((cb, heads, nope), own_heads),
            pl.BlockSpec((cb, heads, vd), own_heads),
        ],
        out_specs=[
            pl.BlockSpec(memory_space=pl.ANY),
            pl.BlockSpec(memory_space=pl.ANY),
            pl.BlockSpec(memory_space=pl.ANY),
            pl.BlockSpec((CBLK, heads * nope), lambda s: (s, 0)),
            pl.BlockSpec((CBLK, heads * (qk - nope)), lambda s: (s, 0)),
            pl.BlockSpec((cb, heads * nope), lambda s: (s, 0)),
            pl.BlockSpec((cb, heads * vd), lambda s: (s, 0)),
        ],
        out_shape=[
            jax.ShapeDtypeStruct((n * kv_own.shape[0], kv_own.shape[1]), bf),
            jax.ShapeDtypeStruct((n * cs_own.shape[0], cs_own.shape[1]), f32),
            jax.ShapeDtypeStruct((n * cq_own.shape[0], rank), bf),
            jax.ShapeDtypeStruct((rank, heads * nope), bf),
            jax.ShapeDtypeStruct((rank, heads * (qk - nope)), bf),
            jax.ShapeDtypeStruct((kv_rank, heads * nope), bf),
            jax.ShapeDtypeStruct((kv_rank, heads * vd), bf),
        ],
        scratch_shapes=[
            pltpu.VMEM((SUB * w_t.shape[2], SUB * heads), bf),
            pltpu.VMEM((CBLK // SUB, SUB * heads, nope), f32),
            pltpu.VMEM((CBLK // SUB, SUB * heads // 2, LANES), f32),
            pltpu.VMEM((2, cb * heads, nope), f32),
            pltpu.SemaphoreType.DMA((3, 11)),
            pltpu.SemaphoreType.DMA((3, 11)),
            pltpu.SemaphoreType.DMA((3,)),
        ],
        compiler_params=pltpu.CompilerParams(collective_id=0, has_side_effects=True, dimension_semantics=("arbitrary",), vmem_limit_bytes=60_000_000),
        cost_estimate=pl.CostEstimate(flops=30_000_000_000, bytes_accessed=90_000_000, transcendentals=0),
        name="gather_pick",
    )(kv_own, cs_own, cq_own, w_t, w_uk, w_uv)


QB = 512
CH = 16


def attn_kernel(scale2, kv_rank, nope, rot, kv_ref, cq_ref, cs_ref, wn_ref, wr_ref, uk_ref, uv_ref, o_ref, kcat, vt, uvt, qcat, acc, mrow, lrow, s0, s1, p0, p1, mx0, mx1, al0, al1):
    b = pl.program_id(0)
    vd = uv_ref.shape[1] // GROUP
    bf = jnp.bfloat16
    sbuf, pbuf, mxb, alb = (s0, s1), (p0, p1), (mx0, mx1), (al0, al1)
    hd = rot // 2
    hb = QB // 2

    @pl.when(b == 0)
    def _():
        uvt[...] = uv_ref[...].T

        def fill(i, _):
            r = pl.ds(pl.multiple_of(i * QB, QB), QB)
            c = kv_ref[r, :kv_rank]
            k = dot_nn(c, uk_ref[...]).astype(bf)
            pe_f = kv_ref[r, kv_rank:kv_rank + LANES].astype(jnp.float32)
            pe = (pe_f.astype(bf), pltpu.roll(pe_f, rot, 1).astype(bf))
            for h in range(GROUP):
                kcat[h, r, :nope] = k[:, h * nope:(h + 1) * nope]
                kcat[h, r, nope:] = pe[h % 2]
            vt[:, r] = dot_nt(uvt[...], c).astype(bf)
            return 0
        lax.fori_loop(0, kv_ref.shape[0] // QB, fill, 0)

    cq = cq_ref[...]
    qn = dot_nn(cq, wn_ref[...]).astype(bf)
    qr = dot_nn(cq, wr_ref[...])
    per = cs_ref.shape[1]
    cos_p, sin_p = [], []
    for j in range(QB // per):
        c_t = cs_ref[j * rot:j * rot + hd, :]
        s_t = cs_ref[j * rot + hd:(j + 1) * rot, :]
        cos_p.append(jnp.concatenate([c_t] * (LANES // hd), axis=0).T)
        sin_p.append(jnp.concatenate([-s_t, s_t] * (LANES // rot), axis=0).T)
    cos_t = jnp.concatenate(cos_p, axis=0)
    sin_t = jnp.concatenate(sin_p, axis=0)
    for pr in range(GROUP // 2):
        z = qr[:, pr * LANES:(pr + 1) * LANES]
        lane = lax.broadcasted_iota(jnp.int32, z.shape, 1)
        swapped = jnp.where((lane // hd) % 2 == 0, pltpu.roll(z, LANES - hd, 1), pltpu.roll(z, hd, 1))
        zr = (z * cos_t + swapped * sin_t).astype(bf)
        for m in range(2):
            h = 2 * pr + m
            qcat[h, :, :nope] = qn[:, h * nope:(h + 1) * nope]
            qcat[h, :, nope:] = zr

    r0 = pl.multiple_of(b * QB, QB)
    tri = lax.broadcasted_iota(jnp.int32, (hb, hb), 0) <= lax.broadcasted_iota(jnp.int32, (hb, hb), 1)

    def score(h, r, slot):
        s = dot_nt(kcat[h, pl.ds(r, QB), :], qcat[h])
        sbuf[slot][...] = s
        mxb[slot][...] = jnp.max(s, axis=0, keepdims=True)

    def soft(h, slot):
        m_old = mrow[h]
        m_new = jnp.maximum(m_old, mxb[slot][...])
        alpha = jnp.exp2((m_old - m_new) * scale2)
        tot = None
        for c in range(0, QB, CH):
            p = jnp.exp2((sbuf[slot][c:c + CH, :] - m_new) * scale2)
            pbuf[slot][c:c + CH, :] = p.astype(bf)
            part = jnp.sum(p.reshape(CH // 8, 8, QB), axis=0)
            tot = part if tot is None else tot + part
        lrow[h] = lrow[h] * alpha + jnp.sum(tot, axis=0, keepdims=True)
        mrow[h] = m_new
        alb[slot][...] = alpha

    def weigh(h, r, slot):
        v = vt[h * vd:(h + 1) * vd, pl.ds(r, QB)]
        acc[h] = acc[h] * alb[slot][...] + dot_nn(v, pbuf[slot][...])

    def score_diag(h, slot):
        k = kcat[h, pl.ds(r0, QB), :]
        q = qcat[h]
        sa = dot_nt(k[:hb], q)
        sa0 = jnp.where(tri, sa[:, :hb], NEG)
        sa1 = sa[:, hb:]
        sb = jnp.where(tri, dot_nt(k[hb:], q[hb:]), NEG)
        sbuf[slot][:hb, :hb] = sa0
        sbuf[slot][:hb, hb:] = sa1
        sbuf[slot][hb:, hb:] = sb
        mxb[slot][:, :hb] = jnp.max(sa0, axis=0, keepdims=True)
        mxb[slot][:, hb:] = jnp.maximum(jnp.max(sa1, axis=0, keepdims=True), jnp.max(sb, axis=0, keepdims=True))

    def soft_diag(h, slot):
        m = mxb[slot][...]
        pa = jnp.exp2((sbuf[slot][:hb, :] - m) * scale2)
        pb = jnp.exp2((sbuf[slot][hb:, hb:] - m[:, hb:]) * scale2)
        pbuf[slot][:hb, :] = pa.astype(bf)
        pbuf[slot][hb:, hb:] = pb.astype(bf)
        la = jnp.sum(pa, axis=0, keepdims=True)
        lrow[h, :, :hb] = la[:, :hb]
        lrow[h, :, hb:] = la[:, hb:] + jnp.sum(pb, axis=0, keepdims=True)
        mrow[h] = m

    def weigh_diag(h, slot):
        rows = slice(h * vd, (h + 1) * vd)
        acc[h, :, :hb] = dot_nn(vt[rows, pl.ds(r0, hb)], pbuf[slot][:hb, :hb])
        acc[h, :, hb:] = dot_nn(vt[rows, pl.ds(r0, QB)], pbuf[slot][:, hb:])

    score_diag(0, 0)
    for h in range(GROUP):
        if h + 1 < GROUP:
            score_diag(h + 1, (h + 1) % 2)
        else:
            score(0, 0, 0)
        soft_diag(h, h % 2)
        weigh_diag(h, h % 2)

    def body(kb, _):
        r = pl.multiple_of(kb * QB, QB)
        for h in range(GROUP):
            if h + 1 < GROUP:
                score(h + 1, r, (h + 1) % 2)
            else:
                score(0, pl.multiple_of(r + QB, QB), 0)
            soft(h, h % 2)
            weigh(h, r, h % 2)
        return 0

    lax.fori_loop(0, b, body, 0)

    for h in range(GROUP):
        o_ref[:, h * vd:(h + 1) * vd] = (acc[h] * (1.0 / lrow[h])).T.astype(bf)


def attention_group(g, scale2, kv_rank, nope, rot, vd, kv_all, cq_all, cs_all, wn, wr, uk, uv):
    seq, rank = cq_all.shape
    bf = jnp.bfloat16
    f32 = jnp.float32
    pairs = seq * (seq + QB) // 2
    blocks = seq // QB
    flops = 2 * GROUP * (seq * rank * (nope + rot) + seq * kv_rank * (nope + vd) + pairs * (nope + rot + vd) * 2)
    row = pltpu.VMEM((1, QB), f32)
    return pl.pallas_call(
        functools.partial(attn_kernel, scale2, kv_rank, nope, rot),
        grid=(blocks,),
        in_specs=[
            pl.BlockSpec(kv_all.shape, lambda b: (0, 0)),
            pl.BlockSpec((QB, rank), lambda b: (b, 0)),
            pl.BlockSpec((cs_all.shape[0] // blocks, cs_all.shape[1]), lambda b: (b, 0)),
            pl.BlockSpec((rank, GROUP * nope), lambda b: (0, g)),
            pl.BlockSpec((rank, GROUP * rot), lambda b: (0, g)),
            pl.BlockSpec((kv_rank, GROUP * nope), lambda b: (0, g)),
            pl.BlockSpec((kv_rank, GROUP * vd), lambda b: (0, g)),
        ],
        out_specs=pl.BlockSpec((QB, GROUP * vd), lambda b: (b, 0)),
        out_shape=jax.ShapeDtypeStruct((seq, GROUP * vd), bf),
        scratch_shapes=[
            pltpu.VMEM((GROUP, seq, nope + LANES), bf),
            pltpu.VMEM((GROUP * vd, seq), bf),
            pltpu.VMEM((GROUP * vd, kv_rank), bf),
            pltpu.VMEM((GROUP, QB, nope + LANES), bf),
            pltpu.VMEM((GROUP, vd, QB), f32),
            pltpu.VMEM((GROUP, 1, QB), f32),
            pltpu.VMEM((GROUP, 1, QB), f32),
            pltpu.VMEM((QB, QB), f32),
            pltpu.VMEM((QB, QB), f32),
            pltpu.VMEM((QB, QB), bf),
            pltpu.VMEM((QB, QB), bf),
            row, row, row, row,
        ],
        compiler_params=pltpu.CompilerParams(dimension_semantics=("arbitrary",), vmem_limit_bytes=60_000_000),
        cost_estimate=pl.CostEstimate(flops=flops, bytes_accessed=12_000_000, transcendentals=pairs * GROUP),
        name="mla_attn",
    )(kv_all, cq_all, cs_all, wn, wr, uk, uv)


NT = 512


def out_kernel(first, *refs):
    if first:
        acc_in, (oa, ob, w_ref, out_ref) = None, refs
    else:
        acc_in, oa, ob, w_ref, out_ref = refs
    n = w_ref.shape[0]
    rows = oa.shape[0] // n
    lhs = jnp.concatenate([o[j * rows:(j + 1) * rows, :] for j in range(n) for o in (oa, ob)], axis=1)
    w = w_ref[...]
    prod = dot_nn(lhs, w.reshape(-1, w.shape[-1]))
    if not first:
        prod = prod + acc_in[...]
    out_ref[...] = prod.astype(out_ref.dtype)


def out_product(acc, oa, ob, w4, call, n):
    seq, width = oa.shape
    rows = seq // n
    hidden = w4.shape[3]
    first = acc is None
    tile = pl.BlockSpec((rows, NT), lambda s: (0, s))
    full = pl.BlockSpec((seq, width), lambda s: (0, 0))
    args = ([] if first else [acc]) + [oa, ob, w4]
    return pl.pallas_call(
        functools.partial(out_kernel, first),
        grid=(hidden // NT,),
        in_specs=([] if first else [tile]) + [full, full, pl.BlockSpec((n, 2, width, NT), lambda s: (0, call, 0, s))],
        out_specs=tile,
        out_shape=jax.ShapeDtypeStruct((rows, hidden), jnp.float32 if first else jnp.bfloat16),
        compiler_params=pltpu.CompilerParams(dimension_semantics=("arbitrary",), vmem_limit_bytes=60_000_000),
        cost_estimate=pl.CostEstimate(flops=4 * rows * hidden * width * n, bytes_accessed=4 * hidden * width * n, transcendentals=0),
        name="out_product",
    )(*args)


def solution(mesh):
    n = mesh.shape['sp']
    rows_spec = P(('dp', 'sp'), None)
    tok_spec = P(('dp', 'sp'))
    rep = P()

    def local_step(tok_in, tok_pos, w_dq, g_q, w_uq, w_dkv, g_kv, w_uk, w_uv, w_o):
        num_heads = w_uq.shape[1]
        heads = num_heads // n
        qk_dim = w_uq.shape[2]
        kv_rank = g_kv.shape[0]
        rot = w_dkv.shape[1] - kv_rank
        nope = qk_dim - rot
        vd = w_uv.shape[2]
        scale2 = (0.1 * math.log(YARN_FACTOR) + 1.0) ** 2 / math.sqrt(qk_dim) / math.log(2.0)

        angles = tok_pos.astype(jnp.float32)[:, None] * rope_freqs(rot)[None, :]
        cos_t, sin_t = jnp.cos(angles), jnp.sin(angles)
        cs_own = jnp.concatenate([cos_t, sin_t], axis=1).T
        cq_own, cache_kv, cache_pe, kv_own = latents(tok_in, w_dq, w_dkv, g_q, g_kv, cos_t, sin_t)

        w_t = jnp.transpose(w_uq, (0, 2, 1))
        kv_all, cs_all, cq_all, wn, wr, uk, uv = gather_and_pick(n, heads, nope, kv_own, cs_own, cq_own, w_t, w_uk, w_uv)

        chunks = heads // GROUP
        o_parts = []
        for g in range(chunks):
            o_g = attention_group(g, scale2, kv_rank, nope, rot, vd, kv_all, cq_all, cs_all, wn, wr, uk, uv)
            o_parts.append(lax.all_to_all(o_g, 'sp', 0, 0, tiled=True))
        w4 = w_o.reshape(n, chunks, GROUP * vd, w_o.shape[2])
        acc = None
        for call in range(chunks // 2):
            acc = out_product(acc, o_parts[2 * call], o_parts[2 * call + 1], w4, call, n)
        return acc, cache_kv, cache_pe

    return jax.shard_map(local_step, mesh=mesh, in_specs=(rows_spec, tok_spec, rep, rep, rep, rep, rep, rep, rep, rep), out_specs=(rows_spec, rows_spec, rows_spec), check_vma=False)
```

```python
import functools
import math
import jax
import jax.numpy as jnp
from jax import lax
from jax.experimental import pallas as pl
from jax.experimental.pallas import tpu as pltpu
from jax.sharding import PartitionSpec as P

ROPE_THETA = 10000.0
YARN_FACTOR = 40.0
ORIG_CTX = 4096.0
BETA_FAST = 32.0
BETA_SLOW = 1.0
NORM_EPS = 1e-6
MESH = pl.DeviceIdType.MESH
LANES = 128
NEG = -1e30
GROUP = 4


def rope_freqs(rot_dim):
    half_dim = rot_dim // 2
    log_base = 2.0 * math.log(ROPE_THETA)
    low_idx = max(math.floor(rot_dim * math.log(ORIG_CTX / (BETA_FAST * 2.0 * math.pi)) / log_base), 0)
    high_idx = min(math.ceil(rot_dim * math.log(ORIG_CTX / (BETA_SLOW * 2.0 * math.pi)) / log_base), half_dim - 1)
    spread = max(high_idx - low_idx, 0.001)
    freq_list = []
    for freq_idx in range(half_dim):
        base_freq = ROPE_THETA ** (-2.0 * freq_idx / rot_dim)
        ramp_val = min(max((freq_idx - low_idx) / spread, 0.0), 1.0)
        freq_list.append(base_freq / YARN_FACTOR * ramp_val + base_freq * (1.0 - ramp_val))
    return jnp.asarray(freq_list, dtype=jnp.float32)


def rotate_half(act_in, cos_t, sin_t):
    half_dim = act_in.shape[-1] // 2
    first = act_in[..., :half_dim]
    second = act_in[..., half_dim:]
    return jnp.concatenate([first * cos_t - second * sin_t, second * cos_t + first * sin_t], axis=-1)


def rms_norm(act_in, gain):
    mean_sq = jnp.mean(act_in * act_in, axis=-1, keepdims=True)
    return act_in * lax.rsqrt(mean_sq + NORM_EPS) * gain


def dot_nt(a, b):
    return lax.dot_general(a, b, (((1,), (1,)), ((), ())), preferred_element_type=jnp.float32)


def dot_nn(a, b):
    return jnp.dot(a, b, preferred_element_type=jnp.float32)


LK = 512
LSLOTS = 6


def latent_kernel(kv_rank, x_ref, wq_ref, wkvt_ref, gq_ref, gkv_ref, cos_ref, sin_ref, cq_ref, kv_ref, pe_ref, own_ref, xb, qb, kb, acc_q, acc_kv, sem):
    bf = jnp.bfloat16
    steps = x_ref.shape[1] // LK

    def copies(s, slot):
        k = pl.ds(pl.multiple_of(s * LK, LK), LK)
        return (
            pltpu.make_async_copy(x_ref.at[:, k], xb.at[slot], sem.at[0, slot]),
            pltpu.make_async_copy(wq_ref.at[k, :], qb.at[slot], sem.at[1, slot]),
            pltpu.make_async_copy(wkvt_ref.at[:, k], kb.at[slot], sem.at[2, slot]),
        )

    for s in range(LSLOTS - 1):
        for c in copies(s, s):
            c.start()
    acc_q[...] = jnp.zeros_like(acc_q)
    acc_kv[...] = jnp.zeros_like(acc_kv)

    def body(s, _):
        slot = lax.rem(s, LSLOTS)

        @pl.when(s + LSLOTS - 1 < steps)
        def _():
            for c in copies(s + LSLOTS - 1, lax.rem(s + LSLOTS - 1, LSLOTS)):
                c.start()
        for c in copies(s, slot):
            c.wait()
        x = xb[slot]
        acc_q[...] += dot_nn(x, qb[slot])
        acc_kv[...] += dot_nt(x, kb[slot])
        return 0

    lax.fori_loop(0, steps, body, 0)
    cq_ref[...] = rms_norm(acc_q[...], gq_ref[...]).astype(bf)
    lat = rms_norm(acc_kv[:, :kv_rank], gkv_ref[...]).astype(bf)
    kv_ref[...] = lat
    pe = rotate_half(acc_kv[:, kv_rank:], cos_ref[...], sin_ref[...]).astype(bf)
    pe_ref[...] = pe
    own_ref[:, :kv_rank] = lat
    own_ref[:, kv_rank:] = jnp.concatenate([pe, jnp.zeros((pe.shape[0], LANES - pe.shape[1]), bf)], axis=1)


def latents(x, w_dq, w_dkv, g_q, g_kv, cos_t, sin_t):
    rows, hidden = x.shape
    rank = w_dq.shape[1]
    kvw = w_dkv.shape[1]
    kv_rank = g_kv.shape[0]
    rot = kvw - kv_rank
    bf = jnp.bfloat16
    anyspec = pl.BlockSpec(memory_space=pl.ANY)
    vm = pl.BlockSpec(memory_space=pltpu.VMEM)
    return pl.pallas_call(
        functools.partial(latent_kernel, kv_rank),
        in_specs=[anyspec] * 3 + [vm] * 4,
        out_specs=[vm] * 4,
        out_shape=[
            jax.ShapeDtypeStruct((rows, rank), bf),
            jax.ShapeDtypeStruct((rows, kv_rank), bf),
            jax.ShapeDtypeStruct((rows, rot), bf),
            jax.ShapeDtypeStruct((rows, kv_rank + LANES), bf),
        ],
        scratch_shapes=[
            pltpu.VMEM((LSLOTS, rows, LK), bf),
            pltpu.VMEM((LSLOTS, LK, rank), bf),
            pltpu.VMEM((LSLOTS, kvw, LK), bf),
            pltpu.VMEM((rows, rank), jnp.float32),
            pltpu.VMEM((rows, kvw), jnp.float32),
            pltpu.SemaphoreType.DMA((3, LSLOTS)),
        ],
        compiler_params=pltpu.CompilerParams(vmem_limit_bytes=60_000_000),
        cost_estimate=pl.CostEstimate(flops=2 * rows * hidden * (rank + kvw), bytes_accessed=2 * hidden * (rank + kvw + rows), transcendentals=0),
        name="latents",
    )(x, w_dq, w_dkv.T, g_q[None, :], g_kv[None, :], cos_t, sin_t)


SUB = 16
CBLK = 192


def gather_kernel(n, heads, nope, kv_ref, cs_ref, cq_ref, wt_ref, uk_ref, uv_ref, kv_all, cs_all, cq_all, wn_ref, wr_ref, uko_ref, uvo_ref, sel, tn, tr, tu, send_sem, recv_sem, loc_sem):
    step = pl.program_id(0)
    last = pl.num_programs(0) - 1
    me = lax.axis_index("sp")
    right = lax.rem(me + 2, n)
    left = lax.rem(me + n - 2, n)
    mate = me + 1 - 2 * lax.rem(me, 2)
    opp = lax.rem(me + 4, n)
    srcs = (kv_ref, cs_ref, cq_ref)
    alls = (kv_all, cs_all, cq_all)
    num = len(srcs)
    bf = jnp.bfloat16

    def piece(arr, owner, part):
        rows = srcs[arr].shape[0]
        half = rows // 2
        off, size = ((0, half), (half, half), (0, rows))[part]
        return alls[arr].at[pl.ds(pl.multiple_of(owner * rows + off, half), size)]

    def own(arr, part):
        half = srcs[arr].shape[0] // 2
        return srcs[arr].at[pl.ds(0, half)] if part == 0 else srcs[arr].at[pl.ds(half, half)] if part == 1 else srcs[arr]

    def rcopy(arr, idx, src, owner, part, dev):
        return pltpu.make_async_remote_copy(
            src_ref=src, dst_ref=piece(arr, owner, part),
            send_sem=send_sem.at[arr, idx], recv_sem=recv_sem.at[arr, idx],
            device_id={"sp": dev}, device_id_type=MESH)

    def copies(arr):
        return [
            rcopy(arr, 0, own(arr, 0), me, 0, right),
            rcopy(arr, 1, own(arr, 1), me, 1, right),
            rcopy(arr, 2, own(arr, 1), me, 1, left),
            rcopy(arr, 3, own(arr, 0), me, 0, left),
            rcopy(arr, 4, own(arr, 2), me, 2, mate),
            rcopy(arr, 5, piece(arr, left, 0), left, 0, right),
            rcopy(arr, 6, piece(arr, right, 1), right, 1, left),
            rcopy(arr, 7, piece(arr, left, 2), left, 2, mate),
            rcopy(arr, 8, piece(arr, right, 2), right, 2, mate),
            rcopy(arr, 9, piece(arr, opp, 0), opp, 0, mate),
            rcopy(arr, 10, piece(arr, opp, 1), opp, 1, mate),
        ]

    cps = [copies(arr) for arr in range(num)]
    loc = [pltpu.make_async_copy(srcs[arr], piece(arr, me, 2), loc_sem.at[arr]) for arr in range(num)]
    width = SUB * heads // 2
    pairs = heads // 2
    lanes = wt_ref.shape[2]

    @pl.when(step == 0)
    def _():
        barrier = pltpu.get_barrier_semaphore()
        for dev in (left, right, mate):
            pl.semaphore_signal(barrier, inc=1, device_id={"sp": dev}, device_id_type=MESH)
        pl.semaphore_wait(barrier, 3)
        for arr in (2, 0, 1):
            for i in (0, 2, 1, 3, 4):
                cps[arr][i].start()
        for arr in range(num):
            loc[arr].start()
        hp = lax.broadcasted_iota(jnp.int32, (lanes, 2 * width), 0)
        col = lax.broadcasted_iota(jnp.int32, (lanes, 2 * width), 1)
        want_h = me * heads + 2 * lax.rem(col, pairs) + col // width
        want_c = lax.rem(col, width) // pairs
        code = jnp.where(hp == want_h, want_c, -1)
        for c in range(SUB):
            sel[c * lanes:(c + 1) * lanes, :] = jnp.where(code == c, 1.0, 0.0).astype(bf)

    def hand_on(arr):
        cps[arr][0].wait_recv()
        cps[arr][5].start()
        cps[arr][2].wait_recv()
        cps[arr][6].start()

    def to_mate(arr):
        cps[arr][1].wait_recv()
        cps[arr][7].start()
        cps[arr][3].wait_recv()
        cps[arr][8].start()

    @pl.when(step == (3 * last) // 7)
    def _():
        hand_on(2)

    @pl.when(step == (5 * last) // 7)
    def _():
        to_mate(2)

    @pl.when(step == last)
    def _():
        hand_on(0)

    for s in range(CBLK // SUB):
        lhs = jnp.concatenate([wt_ref[s * SUB + i] for i in range(SUB)], axis=1)
        g = dot_nn(lhs, sel[...])
        tn[s] = g[:nope].T
        tr[s] = jnp.concatenate([g[nope:, :width], g[nope:, width:]], axis=0).T
        for h in range(heads):
            par, hp = h % 2, h // 2
            wn_ref[s * SUB:(s + 1) * SUB, h * nope:(h + 1) * nope] = tn[s, pl.ds(par * width + hp, SUB, stride=pairs), :].astype(bf)
        for hp in range(pairs):
            wr_ref[s * SUB:(s + 1) * SUB, hp * LANES:(hp + 1) * LANES] = tr[s, pl.ds(hp, SUB, stride=pairs), :].astype(bf)

    cb = uk_ref.shape[0]
    for i, (src, dst) in enumerate(((uk_ref, uko_ref), (uv_ref, uvo_ref))):
        wd = src.shape[2]
        tu[i] = src[...].astype(jnp.float32).reshape(cb * heads, wd)
        for h in range(heads):
            dst[:, h * wd:(h + 1) * wd] = tu[i, pl.ds(h, cb, stride=heads), :].astype(bf)

    @pl.when(step == last)
    def _():
        hand_on(1)
        to_mate(0)
        to_mate(1)
        for arr in (2, 0, 1):
            cps[arr][5].wait_recv()
            cps[arr][9].start()
            cps[arr][6].wait_recv()
            cps[arr][10].start()
        for arr in range(num):
            for i in (4, 7, 8, 9, 10):
                cps[arr][i].wait_recv()
            for i in range(11):
                cps[arr][i].wait_send()
            loc[arr].wait()


def gather_and_pick(n, heads, nope, kv_own, cs_own, cq_own, w_t, w_uk, w_uv):
    rank = cq_own.shape[1]
    qk = w_t.shape[1]
    kv_rank = w_uk.shape[0]
    vd = w_uv.shape[2]
    steps = rank // CBLK
    cb = kv_rank // steps
    bf = jnp.bfloat16
    f32 = jnp.float32
    const = lambda s: (0, 0)
    own_heads = lambda s: (s, lax.axis_index("sp"), 0)
    return pl.pallas_call(
        functools.partial(gather_kernel, n, heads, nope),
        grid=(steps,),
        in_specs=[
            pl.BlockSpec(kv_own.shape, const),
            pl.BlockSpec(cs_own.shape, const),
            pl.BlockSpec(cq_own.shape, const),
            pl.BlockSpec((CBLK, qk, w_t.shape[2]), lambda s: (s, 0, 0)),
            pl.BlockSpec((cb, heads, nope), own_heads),
            pl.BlockSpec((cb, heads, vd), own_heads),
        ],
        out_specs=[
            pl.BlockSpec(memory_space=pl.ANY),
            pl.BlockSpec(memory_space=pl.ANY),
            pl.BlockSpec(memory_space=pl.ANY),
            pl.BlockSpec((CBLK, heads * nope), lambda s: (s, 0)),
            pl.BlockSpec((CBLK, heads * (qk - nope)), lambda s: (s, 0)),
            pl.BlockSpec((cb, heads * nope), lambda s: (s, 0)),
            pl.BlockSpec((cb, heads * vd), lambda s: (s, 0)),
        ],
        out_shape=[
            jax.ShapeDtypeStruct((n * kv_own.shape[0], kv_own.shape[1]), bf),
            jax.ShapeDtypeStruct((n * cs_own.shape[0], cs_own.shape[1]), f32),
            jax.ShapeDtypeStruct((n * cq_own.shape[0], rank), bf),
            jax.ShapeDtypeStruct((rank, heads * nope), bf),
            jax.ShapeDtypeStruct((rank, heads * (qk - nope)), bf),
            jax.ShapeDtypeStruct((kv_rank, heads * nope), bf),
            jax.ShapeDtypeStruct((kv_rank, heads * vd), bf),
        ],
        scratch_shapes=[
            pltpu.VMEM((SUB * w_t.shape[2], SUB * heads), bf),
            pltpu.VMEM((CBLK // SUB, SUB * heads, nope), f32),
            pltpu.VMEM((CBLK // SUB, SUB * heads // 2, LANES), f32),
            pltpu.VMEM((2, cb * heads, nope), f32),
            pltpu.SemaphoreType.DMA((3, 11)),
            pltpu.SemaphoreType.DMA((3, 11)),
            pltpu.SemaphoreType.DMA((3,)),
        ],
        compiler_params=pltpu.CompilerParams(collective_id=0, has_side_effects=True, dimension_semantics=("arbitrary",), vmem_limit_bytes=60_000_000),
        cost_estimate=pl.CostEstimate(flops=30_000_000_000, bytes_accessed=90_000_000, transcendentals=0),
        name="gather_pick",
    )(kv_own, cs_own, cq_own, w_t, w_uk, w_uv)


QB = 512
CH = 16


def attn_kernel(scale2, kv_rank, nope, rot, kv_ref, cq_ref, cs_ref, wn_ref, wr_ref, uk_ref, uv_ref, o_ref, kcat, vt, uvt, qcat, acc, mrow, lrow, s0, s1, p0, p1, mx0, mx1, al0, al1):
    b = pl.program_id(0)
    vd = uv_ref.shape[1] // GROUP
    bf = jnp.bfloat16
    sbuf, pbuf, mxb, alb = (s0, s1), (p0, p1), (mx0, mx1), (al0, al1)
    hd = rot // 2
    hb = QB // 2

    @pl.when(b == 0)
    def _():
        uvt[...] = uv_ref[...].T

        def fill(i, _):
            r = pl.ds(pl.multiple_of(i * QB, QB), QB)
            c = kv_ref[r, :kv_rank]
            k = dot_nn(c, uk_ref[...]).astype(bf)
            pe_f = kv_ref[r, kv_rank:kv_rank + LANES].astype(jnp.float32)
            pe = (pe_f.astype(bf), pltpu.roll(pe_f, rot, 1).astype(bf))
            for h in range(GROUP):
                kcat[h, r, :nope] = k[:, h * nope:(h + 1) * nope]
                kcat[h, r, nope:] = pe[h % 2]
            vt[:, r] = dot_nt(uvt[...], c).astype(bf)
            return 0
        lax.fori_loop(0, kv_ref.shape[0] // QB, fill, 0)

    cq = cq_ref[...]
    qn = dot_nn(cq, wn_ref[...]).astype(bf)
    qr = dot_nn(cq, wr_ref[...])
    per = cs_ref.shape[1]
    cos_p, sin_p = [], []
    for j in range(QB // per):
        c_t = cs_ref[j * rot:j * rot + hd, :]
        s_t = cs_ref[j * rot + hd:(j + 1) * rot, :]
        cos_p.append(jnp.concatenate([c_t] * (LANES // hd), axis=0).T)
        sin_p.append(jnp.concatenate([-s_t, s_t] * (LANES // rot), axis=0).T)
    cos_t = jnp.concatenate(cos_p, axis=0)
    sin_t = jnp.concatenate(sin_p, axis=0)
    for pr in range(GROUP // 2):
        z = qr[:, pr * LANES:(pr + 1) * LANES]
        lane = lax.broadcasted_iota(jnp.int32, z.shape, 1)
        swapped = jnp.where((lane // hd) % 2 == 0, pltpu.roll(z, LANES - hd, 1), pltpu.roll(z, hd, 1))
        zr = (z * cos_t + swapped * sin_t).astype(bf)
        for m in range(2):
            h = 2 * pr + m
            qcat[h, :, :nope] = qn[:, h * nope:(h + 1) * nope]
            qcat[h, :, nope:] = zr

    r0 = pl.multiple_of(b * QB, QB)
    tri = lax.broadcasted_iota(jnp.int32, (hb, hb), 0) <= lax.broadcasted_iota(jnp.int32, (hb, hb), 1)

    def score(h, r, slot):
        s = dot_nt(kcat[h, pl.ds(r, QB), :], qcat[h])
        sbuf[slot][...] = s
        mxb[slot][...] = jnp.max(s, axis=0, keepdims=True)

    def soft(h, slot):
        m_old = mrow[h]
        m_new = jnp.maximum(m_old, mxb[slot][...])
        alpha = jnp.exp2((m_old - m_new) * scale2)
        tot = None
        for c in range(0, QB, CH):
            p = jnp.exp2((sbuf[slot][c:c + CH, :] - m_new) * scale2)
            pbuf[slot][c:c + CH, :] = p.astype(bf)
            part = jnp.sum(p.reshape(CH // 8, 8, QB), axis=0)
            tot = part if tot is None else tot + part
        lrow[h] = lrow[h] * alpha + jnp.sum(tot, axis=0, keepdims=True)
        mrow[h] = m_new
        alb[slot][...] = alpha

    def weigh(h, r, slot):
        v = vt[h * vd:(h + 1) * vd, pl.ds(r, QB)]
        acc[h] = acc[h] * alb[slot][...] + dot_nn(v, pbuf[slot][...])

    def score_diag(h, slot):
        k = kcat[h, pl.ds(r0, QB), :]
        q = qcat[h]
        sa = dot_nt(k[:hb], q)
        sa0 = jnp.where(tri, sa[:, :hb], NEG)
        sa1 = sa[:, hb:]
        sb = jnp.where(tri, dot_nt(k[hb:], q[hb:]), NEG)
        sbuf[slot][:hb, :hb] = sa0
        sbuf[slot][:hb, hb:] = sa1
        sbuf[slot][hb:, hb:] = sb
        mxb[slot][:, :hb] = jnp.max(sa0, axis=0, keepdims=True)
        mxb[slot][:, hb:] = jnp.maximum(jnp.max(sa1, axis=0, keepdims=True), jnp.max(sb, axis=0, keepdims=True))

    def soft_diag(h, slot):
        m = mxb[slot][...]
        pa = jnp.exp2((sbuf[slot][:hb, :] - m) * scale2)
        pb = jnp.exp2((sbuf[slot][hb:, hb:] - m[:, hb:]) * scale2)
        pbuf[slot][:hb, :] = pa.astype(bf)
        pbuf[slot][hb:, hb:] = pb.astype(bf)
        la = jnp.sum(pa, axis=0, keepdims=True)
        lrow[h, :, :hb] = la[:, :hb]
        lrow[h, :, hb:] = la[:, hb:] + jnp.sum(pb, axis=0, keepdims=True)
        mrow[h] = m

    def weigh_diag(h, slot):
        rows = slice(h * vd, (h + 1) * vd)
        acc[h, :, :hb] = dot_nn(vt[rows, pl.ds(r0, hb)], pbuf[slot][:hb, :hb])
        acc[h, :, hb:] = dot_nn(vt[rows, pl.ds(r0, QB)], pbuf[slot][:, hb:])

    score_diag(0, 0)
    for h in range(GROUP):
        if h + 1 < GROUP:
            score_diag(h + 1, (h + 1) % 2)
        else:
            score(0, 0, 0)
        soft_diag(h, h % 2)
        weigh_diag(h, h % 2)

    def body(kb, _):
        r = pl.multiple_of(kb * QB, QB)
        for h in range(GROUP):
            if h + 1 < GROUP:
                score(h + 1, r, (h + 1) % 2)
            else:
                score(0, pl.multiple_of(r + QB, QB), 0)
            soft(h, h % 2)
            weigh(h, r, h % 2)
        return 0

    lax.fori_loop(0, b, body, 0)

    for h in range(GROUP):
        o_ref[:, h * vd:(h + 1) * vd] = (acc[h] * (1.0 / lrow[h])).T.astype(bf)


def attention_group(g, scale2, kv_rank, nope, rot, vd, kv_all, cq_all, cs_all, wn, wr, uk, uv):
    seq, rank = cq_all.shape
    bf = jnp.bfloat16
    f32 = jnp.float32
    pairs = seq * (seq + QB) // 2
    blocks = seq // QB
    flops = 2 * GROUP * (seq * rank * (nope + rot) + seq * kv_rank * (nope + vd) + pairs * (nope + rot + vd) * 2)
    row = pltpu.VMEM((1, QB), f32)
    return pl.pallas_call(
        functools.partial(attn_kernel, scale2, kv_rank, nope, rot),
        grid=(blocks,),
        in_specs=[
            pl.BlockSpec(kv_all.shape, lambda b: (0, 0)),
            pl.BlockSpec((QB, rank), lambda b: (b, 0)),
            pl.BlockSpec((cs_all.shape[0] // blocks, cs_all.shape[1]), lambda b: (b, 0)),
            pl.BlockSpec((rank, GROUP * nope), lambda b: (0, g)),
            pl.BlockSpec((rank, GROUP * rot), lambda b: (0, g)),
            pl.BlockSpec((kv_rank, GROUP * nope), lambda b: (0, g)),
            pl.BlockSpec((kv_rank, GROUP * vd), lambda b: (0, g)),
        ],
        out_specs=pl.BlockSpec((QB, GROUP * vd), lambda b: (b, 0)),
        out_shape=jax.ShapeDtypeStruct((seq, GROUP * vd), bf),
        scratch_shapes=[
            pltpu.VMEM((GROUP, seq, nope + LANES), bf),
            pltpu.VMEM((GROUP * vd, seq), bf),
            pltpu.VMEM((GROUP * vd, kv_rank), bf),
            pltpu.VMEM((GROUP, QB, nope + LANES), bf),
            pltpu.VMEM((GROUP, vd, QB), f32),
            pltpu.VMEM((GROUP, 1, QB), f32),
            pltpu.VMEM((GROUP, 1, QB), f32),
            pltpu.VMEM((QB, QB), f32),
            pltpu.VMEM((QB, QB), f32),
            pltpu.VMEM((QB, QB), bf),
            pltpu.VMEM((QB, QB), bf),
            row, row, row, row,
        ],
        compiler_params=pltpu.CompilerParams(dimension_semantics=("arbitrary",), vmem_limit_bytes=60_000_000),
        cost_estimate=pl.CostEstimate(flops=flops, bytes_accessed=12_000_000, transcendentals=pairs * GROUP),
        name="mla_attn",
    )(kv_all, cq_all, cs_all, wn, wr, uk, uv)


OSLOTS = 3
NT = 1024


def out_kernel(n, call, first, *refs):
    if first:
        oa, ob, w_ref, out_ref, wbuf, acc, sem, acc_sem = refs
    else:
        acc_in, oa, ob, w_ref, out_ref, wbuf, acc, sem, acc_sem = refs
    rows = oa.shape[0] // n
    hidden = w_ref.shape[3]
    steps = 2 * n

    def copy(s, slot):
        return pltpu.make_async_copy(w_ref.at[lax.rem(s, n), 2 * call + s // n], wbuf.at[slot], sem.at[slot])

    for s in range(OSLOTS - 1):
        copy(s, s).start()
    if first:
        acc[...] = jnp.zeros_like(acc)
    else:
        pltpu.make_async_copy(acc_in, acc, acc_sem).start()
        pltpu.make_async_copy(acc_in, acc, acc_sem).wait()

    def body(s, _):
        slot = lax.rem(s, OSLOTS)

        @pl.when(s + OSLOTS - 1 < steps)
        def _():
            copy(s + OSLOTS - 1, lax.rem(s + OSLOTS - 1, OSLOTS)).start()
        copy(s, slot).wait()
        r = pl.ds(pl.multiple_of(lax.rem(s, n) * rows, rows), rows)
        lhs = jnp.where(s < n, oa[r, :], ob[r, :])
        for t in range(hidden // NT):
            cols = slice(t * NT, (t + 1) * NT)
            acc[:, cols] += dot_nn(lhs, wbuf[slot, :, cols])
        return 0

    lax.fori_loop(0, steps, body, 0)
    if first:
        pltpu.make_async_copy(acc, out_ref, acc_sem).start()
        pltpu.make_async_copy(acc, out_ref, acc_sem).wait()
    else:
        out_ref[...] = acc[...].astype(out_ref.dtype)


def out_product(acc, oa, ob, w4, call, n):
    seq, width = oa.shape
    rows = seq // n
    hidden = w4.shape[3]
    first = acc is None
    anyspec = pl.BlockSpec(memory_space=pl.ANY)
    vm = pl.BlockSpec(memory_space=pltpu.VMEM)
    args = ([] if first else [acc]) + [oa, ob, w4]
    return pl.pallas_call(
        functools.partial(out_kernel, n, call, first),
        in_specs=([] if first else [anyspec]) + [vm, vm, anyspec],
        out_specs=anyspec if first else vm,
        out_shape=jax.ShapeDtypeStruct((rows, hidden), jnp.float32 if first else jnp.bfloat16),
        scratch_shapes=[
            pltpu.VMEM((OSLOTS, width, hidden), jnp.bfloat16),
            pltpu.VMEM((rows, hidden), jnp.float32),
            pltpu.SemaphoreType.DMA((OSLOTS,)),
            pltpu.SemaphoreType.DMA,
        ],
        compiler_params=pltpu.CompilerParams(vmem_limit_bytes=60_000_000),
        cost_estimate=pl.CostEstimate(flops=4 * rows * hidden * width * n, bytes_accessed=4 * hidden * width * n, transcendentals=0),
        name="out_product",
    )(*args)


def solution(mesh):
    n = mesh.shape['sp']
    rows_spec = P(('dp', 'sp'), None)
    tok_spec = P(('dp', 'sp'))
    rep = P()

    def local_step(tok_in, tok_pos, w_dq, g_q, w_uq, w_dkv, g_kv, w_uk, w_uv, w_o):
        num_heads = w_uq.shape[1]
        heads = num_heads // n
        qk_dim = w_uq.shape[2]
        kv_rank = g_kv.shape[0]
        rot = w_dkv.shape[1] - kv_rank
        nope = qk_dim - rot
        vd = w_uv.shape[2]
        scale2 = (0.1 * math.log(YARN_FACTOR) + 1.0) ** 2 / math.sqrt(qk_dim) / math.log(2.0)

        angles = tok_pos.astype(jnp.float32)[:, None] * rope_freqs(rot)[None, :]
        cos_t, sin_t = jnp.cos(angles), jnp.sin(angles)
        cs_own = jnp.concatenate([cos_t, sin_t], axis=1).T
        cq_own, cache_kv, cache_pe, kv_own = latents(tok_in, w_dq, w_dkv, g_q, g_kv, cos_t, sin_t)

        w_t = jnp.transpose(w_uq, (0, 2, 1))
        kv_all, cs_all, cq_all, wn, wr, uk, uv = gather_and_pick(n, heads, nope, kv_own, cs_own, cq_own, w_t, w_uk, w_uv)

        chunks = heads // GROUP
        o_parts = []
        for g in range(chunks):
            o_g = attention_group(g, scale2, kv_rank, nope, rot, vd, kv_all, cq_all, cs_all, wn, wr, uk, uv)
            o_parts.append(lax.all_to_all(o_g, 'sp', 0, 0, tiled=True))
        w4 = w_o.reshape(n, chunks, GROUP * vd, w_o.shape[2])
        acc = None
        for call in range(chunks // 2):
            acc = out_product(acc, o_parts[2 * call], o_parts[2 * call + 1], w4, call, n)
        return acc, cache_kv, cache_pe

    return jax.shard_map(local_step, mesh=mesh, in_specs=(rows_spec, tok_spec, rep, rep, rep, rep, rep, rep, rep, rep), out_specs=(rows_spec, rows_spec, rows_spec), check_vma=False)
```

```python
import functools
import math
import jax
import jax.numpy as jnp
from jax import lax
from jax.experimental import pallas as pl
from jax.experimental.pallas import tpu as pltpu
from jax.sharding import PartitionSpec as P

ROPE_THETA = 10000.0
YARN_FACTOR = 40.0
ORIG_CTX = 4096.0
BETA_FAST = 32.0
BETA_SLOW = 1.0
NORM_EPS = 1e-6
MESH = pl.DeviceIdType.MESH
LANES = 128
NEG = -1e30
GROUP = 8


def rope_freqs(rot_dim):
    half_dim = rot_dim // 2
    log_base = 2.0 * math.log(ROPE_THETA)
    low_idx = max(math.floor(rot_dim * math.log(ORIG_CTX / (BETA_FAST * 2.0 * math.pi)) / log_base), 0)
    high_idx = min(math.ceil(rot_dim * math.log(ORIG_CTX / (BETA_SLOW * 2.0 * math.pi)) / log_base), half_dim - 1)
    spread = max(high_idx - low_idx, 0.001)
    freq_list = []
    for freq_idx in range(half_dim):
        base_freq = ROPE_THETA ** (-2.0 * freq_idx / rot_dim)
        ramp_val = min(max((freq_idx - low_idx) / spread, 0.0), 1.0)
        freq_list.append(base_freq / YARN_FACTOR * ramp_val + base_freq * (1.0 - ramp_val))
    return jnp.asarray(freq_list, dtype=jnp.float32)


def rotate_half(act_in, cos_t, sin_t):
    half_dim = act_in.shape[-1] // 2
    first = act_in[..., :half_dim]
    second = act_in[..., half_dim:]
    return jnp.concatenate([first * cos_t - second * sin_t, second * cos_t + first * sin_t], axis=-1)


def rms_norm(act_in, gain):
    mean_sq = jnp.mean(act_in * act_in, axis=-1, keepdims=True)
    return act_in * lax.rsqrt(mean_sq + NORM_EPS) * gain


def dot_nt(a, b):
    return lax.dot_general(a, b, (((1,), (1,)), ((), ())), preferred_element_type=jnp.float32)


def dot_nn(a, b):
    return jnp.dot(a, b, preferred_element_type=jnp.float32)


LK = 512
LSLOTS = 6


def latent_kernel(kv_rank, x_ref, wq_ref, wkvt_ref, gq_ref, gkv_ref, cs_ref, cq_ref, kv_ref, pe_ref, own_ref, xb, qb, kb, acc_q, acc_kv, sem):
    bf = jnp.bfloat16
    steps = x_ref.shape[1] // LK

    def copies(s, slot):
        k = pl.ds(pl.multiple_of(s * LK, LK), LK)
        return (
            pltpu.make_async_copy(x_ref.at[:, k], xb.at[slot], sem.at[0, slot]),
            pltpu.make_async_copy(wq_ref.at[k, :], qb.at[slot], sem.at[1, slot]),
            pltpu.make_async_copy(wkvt_ref.at[:, k], kb.at[slot], sem.at[2, slot]),
        )

    for s in range(LSLOTS - 1):
        for c in copies(s, s):
            c.start()
    acc_q[...] = jnp.zeros_like(acc_q)
    acc_kv[...] = jnp.zeros_like(acc_kv)

    def body(s, _):
        slot = lax.rem(s, LSLOTS)

        @pl.when(s + LSLOTS - 1 < steps)
        def _():
            for c in copies(s + LSLOTS - 1, lax.rem(s + LSLOTS - 1, LSLOTS)):
                c.start()
        for c in copies(s, slot):
            c.wait()
        x = xb[slot]
        acc_q[...] += dot_nn(x, qb[slot])
        acc_kv[...] += dot_nt(x, kb[slot])
        return 0

    lax.fori_loop(0, steps, body, 0)
    cq_ref[...] = rms_norm(acc_q[...], gq_ref[...]).astype(bf)
    lat = rms_norm(acc_kv[:, :kv_rank], gkv_ref[...]).astype(bf)
    kv_ref[...] = lat
    cs = cs_ref[...].T
    half = cs.shape[1] // 2
    pe = rotate_half(acc_kv[:, kv_rank:], cs[:, :half], cs[:, half:]).astype(bf)
    pe_ref[...] = pe
    own_ref[:, :kv_rank] = lat
    own_ref[:, kv_rank:] = jnp.concatenate([pe, jnp.zeros((pe.shape[0], LANES - pe.shape[1]), bf)], axis=1)


def latents(x, w_dq, w_dkv, g_q, g_kv, cs_own):
    rows, hidden = x.shape
    rank = w_dq.shape[1]
    kvw = w_dkv.shape[1]
    kv_rank = g_kv.shape[0]
    rot = kvw - kv_rank
    bf = jnp.bfloat16
    anyspec = pl.BlockSpec(memory_space=pl.ANY)
    vm = pl.BlockSpec(memory_space=pltpu.VMEM)
    return pl.pallas_call(
        functools.partial(latent_kernel, kv_rank),
        in_specs=[anyspec] * 3 + [vm] * 3,
        out_specs=[vm] * 4,
        out_shape=[
            jax.ShapeDtypeStruct((rows, rank), bf),
            jax.ShapeDtypeStruct((rows, kv_rank), bf),
            jax.ShapeDtypeStruct((rows, rot), bf),
            jax.ShapeDtypeStruct((rows, kv_rank + LANES), bf),
        ],
        scratch_shapes=[
            pltpu.VMEM((LSLOTS, rows, LK), bf),
            pltpu.VMEM((LSLOTS, LK, rank), bf),
            pltpu.VMEM((LSLOTS, kvw, LK), bf),
            pltpu.VMEM((rows, rank), jnp.float32),
            pltpu.VMEM((rows, kvw), jnp.float32),
            pltpu.SemaphoreType.DMA((3, LSLOTS)),
        ],
        compiler_params=pltpu.CompilerParams(vmem_limit_bytes=60_000_000),
        cost_estimate=pl.CostEstimate(flops=2 * rows * hidden * (rank + kvw), bytes_accessed=2 * hidden * (rank + kvw + rows), transcendentals=0),
        name="latents",
    )(x, w_dq, w_dkv.T, g_q[None, :], g_kv[None, :], cs_own)


SUB = 16
CBLK = 192


def gather_kernel(n, heads, nope, kv_ref, cs_ref, cq_ref, wt_ref, uk_ref, uv_ref, kv_all, cs_all, cq_all, wn_ref, wr_ref, uko_ref, uvo_ref, sel, tn, tr, tu, send_sem, recv_sem, loc_sem):
    step = pl.program_id(0)
    last = pl.num_programs(0) - 1
    me = lax.axis_index("sp")
    right = lax.rem(me + 2, n)
    left = lax.rem(me + n - 2, n)
    mate = me + 1 - 2 * lax.rem(me, 2)
    opp = lax.rem(me + 4, n)
    srcs = (kv_ref, cs_ref, cq_ref)
    alls = (kv_all, cs_all, cq_all)
    num = len(srcs)
    bf = jnp.bfloat16

    def piece(arr, owner, part):
        rows = srcs[arr].shape[0]
        half = rows // 2
        off, size = ((0, half), (half, half), (0, rows))[part]
        return alls[arr].at[pl.ds(pl.multiple_of(owner * rows + off, half), size)]

    def own(arr, part):
        half = srcs[arr].shape[0] // 2
        return srcs[arr].at[pl.ds(0, half)] if part == 0 else srcs[arr].at[pl.ds(half, half)] if part == 1 else srcs[arr]

    def rcopy(arr, idx, src, owner, part, dev):
        return pltpu.make_async_remote_copy(
            src_ref=src, dst_ref=piece(arr, owner, part),
            send_sem=send_sem.at[arr, idx], recv_sem=recv_sem.at[arr, idx],
            device_id={"sp": dev}, device_id_type=MESH)

    def copies(arr):
        return [
            rcopy(arr, 0, own(arr, 0), me, 0, right),
            rcopy(arr, 1, own(arr, 1), me, 1, right),
            rcopy(arr, 2, own(arr, 1), me, 1, left),
            rcopy(arr, 3, own(arr, 0), me, 0, left),
            rcopy(arr, 4, own(arr, 2), me, 2, mate),
            rcopy(arr, 5, piece(arr, left, 0), left, 0, right),
            rcopy(arr, 6, piece(arr, right, 1), right, 1, left),
            rcopy(arr, 7, piece(arr, left, 2), left, 2, mate),
            rcopy(arr, 8, piece(arr, right, 2), right, 2, mate),
            rcopy(arr, 9, piece(arr, opp, 0), opp, 0, mate),
            rcopy(arr, 10, piece(arr, opp, 1), opp, 1, mate),
        ]

    cps = [copies(arr) for arr in range(num)]
    loc = [pltpu.make_async_copy(srcs[arr], piece(arr, me, 2), loc_sem.at[arr]) for arr in range(num)]
    width = SUB * heads // 2
    pairs = heads // 2
    lanes = wt_ref.shape[2]

    @pl.when(step == 0)
    def _():
        barrier = pltpu.get_barrier_semaphore()
        for dev in (left, right, mate):
            pl.semaphore_signal(barrier, inc=1, device_id={"sp": dev}, device_id_type=MESH)
        pl.semaphore_wait(barrier, 3)
        for arr in (2, 0, 1):
            for i in (0, 2, 1, 3, 4):
                cps[arr][i].start()
        for arr in range(num):
            loc[arr].start()
        hp = lax.broadcasted_iota(jnp.int32, (lanes, 2 * width), 0)
        col = lax.broadcasted_iota(jnp.int32, (lanes, 2 * width), 1)
        want_h = me * heads + 2 * lax.rem(col, pairs) + col // width
        want_c = lax.rem(col, width) // pairs
        code = jnp.where(hp == want_h, want_c, -1)
        for c in range(SUB):
            sel[c * lanes:(c + 1) * lanes, :] = jnp.where(code == c, 1.0, 0.0).astype(bf)

    def hand_on(arr):
        cps[arr][0].wait_recv()
        cps[arr][5].start()
        cps[arr][2].wait_recv()
        cps[arr][6].start()

    def to_mate(arr):
        cps[arr][1].wait_recv()
        cps[arr][7].start()
        cps[arr][3].wait_recv()
        cps[arr][8].start()

    @pl.when(step == (3 * last) // 7)
    def _():
        hand_on(2)

    @pl.when(step == (5 * last) // 7)
    def _():
        to_mate(2)

    @pl.when(step == last)
    def _():
        hand_on(0)

    for s in range(CBLK // SUB):
        lhs = jnp.concatenate([wt_ref[s * SUB + i] for i in range(SUB)], axis=1)
        g = dot_nn(lhs, sel[...])
        tn[s] = g[:nope].T
        tr[s] = jnp.concatenate([g[nope:, :width], g[nope:, width:]], axis=0).T
        for h in range(heads):
            par, hp = h % 2, h // 2
            wn_ref[s * SUB:(s + 1) * SUB, h * nope:(h + 1) * nope] = tn[s, pl.ds(par * width + hp, SUB, stride=pairs), :].astype(bf)
        for hp in range(pairs):
            wr_ref[s * SUB:(s + 1) * SUB, hp * LANES:(hp + 1) * LANES] = tr[s, pl.ds(hp, SUB, stride=pairs), :].astype(bf)

    cb = uk_ref.shape[0]
    for i, (src, dst) in enumerate(((uk_ref, uko_ref), (uv_ref, uvo_ref))):
        wd = src.shape[2]
        tu[i] = src[...].astype(jnp.float32).reshape(cb * heads, wd)
        for h in range(heads):
            dst[:, h * wd:(h + 1) * wd] = tu[i, pl.ds(h, cb, stride=heads), :].astype(bf)

    @pl.when(step == last)
    def _():
        hand_on(1)
        to_mate(0)
        to_mate(1)
        for arr in (2, 0, 1):
            cps[arr][5].wait_recv()
            cps[arr][9].start()
            cps[arr][6].wait_recv()
            cps[arr][10].start()
        for arr in range(num):
            for i in (4, 7, 8, 9, 10):
                cps[arr][i].wait_recv()
            for i in range(11):
                cps[arr][i].wait_send()
            loc[arr].wait()


def gather_and_pick(n, heads, nope, kv_own, cs_own, cq_own, w_t, w_uk, w_uv):
    rank = cq_own.shape[1]
    qk = w_t.shape[1]
    kv_rank = w_uk.shape[0]
    vd = w_uv.shape[2]
    steps = rank // CBLK
    cb = kv_rank // steps
    bf = jnp.bfloat16
    f32 = jnp.float32
    const = lambda s: (0, 0)
    own_heads = lambda s: (s, lax.axis_index("sp"), 0)
    return pl.pallas_call(
        functools.partial(gather_kernel, n, heads, nope),
        grid=(steps,),
        in_specs=[
            pl.BlockSpec(kv_own.shape, const),
            pl.BlockSpec(cs_own.shape, const),
            pl.BlockSpec(cq_own.shape, const),
            pl.BlockSpec((CBLK, qk, w_t.shape[2]), lambda s: (s, 0, 0)),
            pl.BlockSpec((cb, heads, nope), own_heads),
            pl.BlockSpec((cb, heads, vd), own_heads),
        ],
        out_specs=[
            pl.BlockSpec(memory_space=pl.ANY),
            pl.BlockSpec(memory_space=pl.ANY),
            pl.BlockSpec(memory_space=pl.ANY),
            pl.BlockSpec((CBLK, heads * nope), lambda s: (s, 0)),
            pl.BlockSpec((CBLK, heads * (qk - nope)), lambda s: (s, 0)),
            pl.BlockSpec((cb, heads * nope), lambda s: (s, 0)),
            pl.BlockSpec((cb, heads * vd), lambda s: (s, 0)),
        ],
        out_shape=[
            jax.ShapeDtypeStruct((n * kv_own.shape[0], kv_own.shape[1]), bf),
            jax.ShapeDtypeStruct((n * cs_own.shape[0], cs_own.shape[1]), f32),
            jax.ShapeDtypeStruct((n * cq_own.shape[0], rank), bf),
            jax.ShapeDtypeStruct((rank, heads * nope), bf),
            jax.ShapeDtypeStruct((rank, heads * (qk - nope)), bf),
            jax.ShapeDtypeStruct((kv_rank, heads * nope), bf),
            jax.ShapeDtypeStruct((kv_rank, heads * vd), bf),
        ],
        scratch_shapes=[
            pltpu.VMEM((SUB * w_t.shape[2], SUB * heads), bf),
            pltpu.VMEM((CBLK // SUB, SUB * heads, nope), f32),
            pltpu.VMEM((CBLK // SUB, SUB * heads // 2, LANES), f32),
            pltpu.VMEM((2, cb * heads, nope), f32),
            pltpu.SemaphoreType.DMA((3, 11)),
            pltpu.SemaphoreType.DMA((3, 11)),
            pltpu.SemaphoreType.DMA((3,)),
        ],
        compiler_params=pltpu.CompilerParams(collective_id=0, has_side_effects=True, dimension_semantics=("arbitrary",), vmem_limit_bytes=60_000_000),
        cost_estimate=pl.CostEstimate(flops=30_000_000_000, bytes_accessed=90_000_000, transcendentals=0),
        name="gather_pick",
    )(kv_own, cs_own, cq_own, w_t, w_uk, w_uv)


QB = 512
CH = 16


def attn_kernel(scale2, kv_rank, nope, rot, kv_ref, cq_ref, cs_ref, wn_ref, wr_ref, uk_ref, uv_ref, o_ref, kcat, vt, uvt, qcat, acc, mrow, lrow, s0, s1, p0, p1, mx0, mx1, al0, al1):
    b = pl.program_id(0)
    vd = uv_ref.shape[1] // GROUP
    bf = jnp.bfloat16
    sbuf, pbuf, mxb, alb = (s0, s1), (p0, p1), (mx0, mx1), (al0, al1)
    hd = rot // 2
    hb = QB // 2

    @pl.when(b == 0)
    def _():
        uvt[...] = uv_ref[...].T

        def fill(i, _):
            r = pl.ds(pl.multiple_of(i * QB, QB), QB)
            c = kv_ref[r, :kv_rank]
            k = dot_nn(c, uk_ref[...]).astype(bf)
            pe_f = kv_ref[r, kv_rank:kv_rank + LANES].astype(jnp.float32)
            pe = (pe_f.astype(bf), pltpu.roll(pe_f, rot, 1).astype(bf))
            for h in range(GROUP):
                kcat[h, r, :nope] = k[:, h * nope:(h + 1) * nope]
                kcat[h, r, nope:] = pe[h % 2]
            vt[:, r] = dot_nt(uvt[...], c).astype(bf)
            return 0
        lax.fori_loop(0, kv_ref.shape[0] // QB, fill, 0)

    cq = cq_ref[...]
    qn = dot_nn(cq, wn_ref[...]).astype(bf)
    qr = dot_nn(cq, wr_ref[...])
    per = cs_ref.shape[1]
    cos_p, sin_p = [], []
    for j in range(QB // per):
        c_t = cs_ref[j * rot:j * rot + hd, :]
        s_t = cs_ref[j * rot + hd:(j + 1) * rot, :]
        cos_p.append(jnp.concatenate([c_t] * (LANES // hd), axis=0).T)
        sin_p.append(jnp.concatenate([-s_t, s_t] * (LANES // rot), axis=0).T)
    cos_t = jnp.concatenate(cos_p, axis=0)
    sin_t = jnp.concatenate(sin_p, axis=0)
    for pr in range(GROUP // 2):
        z = qr[:, pr * LANES:(pr + 1) * LANES]
        lane = lax.broadcasted_iota(jnp.int32, z.shape, 1)
        swapped = jnp.where((lane // hd) % 2 == 0, pltpu.roll(z, LANES - hd, 1), pltpu.roll(z, hd, 1))
        zr = (z * cos_t + swapped * sin_t).astype(bf)
        for m in range(2):
            h = 2 * pr + m
            qcat[h, :, :nope] = qn[:, h * nope:(h + 1) * nope]
            qcat[h, :, nope:] = zr

    r0 = pl.multiple_of(b * QB, QB)
    tri = lax.broadcasted_iota(jnp.int32, (hb, hb), 0) <= lax.broadcasted_iota(jnp.int32, (hb, hb), 1)

    def score(h, r, slot):
        s = dot_nt(kcat[h, pl.ds(r, QB), :], qcat[h])
        sbuf[slot][...] = s
        mxb[slot][...] = jnp.max(s, axis=0, keepdims=True)

    def soft(h, slot):
        m_old = mrow[h]
        m_new = jnp.maximum(m_old, mxb[slot][...])
        alpha = jnp.exp2((m_old - m_new) * scale2)
        tot = None
        for c in range(0, QB, CH):
            p = jnp.exp2((sbuf[slot][c:c + CH, :] - m_new) * scale2)
            pbuf[slot][c:c + CH, :] = p.astype(bf)
            part = jnp.sum(p.reshape(CH // 8, 8, QB), axis=0)
            tot = part if tot is None else tot + part
        lrow[h] = lrow[h] * alpha + jnp.sum(tot, axis=0, keepdims=True)
        mrow[h] = m_new
        alb[slot][...] = alpha

    def weigh(h, r, slot):
        v = vt[h * vd:(h + 1) * vd, pl.ds(r, QB)]
        acc[h] = acc[h] * alb[slot][...] + dot_nn(v, pbuf[slot][...])

    def score_diag(h, slot):
        k = kcat[h, pl.ds(r0, QB), :]
        q = qcat[h]
        sa = dot_nt(k[:hb], q)
        sa0 = jnp.where(tri, sa[:, :hb], NEG)
        sa1 = sa[:, hb:]
        sb = jnp.where(tri, dot_nt(k[hb:], q[hb:]), NEG)
        sbuf[slot][:hb, :hb] = sa0
        sbuf[slot][:hb, hb:] = sa1
        sbuf[slot][hb:, hb:] = sb
        mxb[slot][:, :hb] = jnp.max(sa0, axis=0, keepdims=True)
        mxb[slot][:, hb:] = jnp.maximum(jnp.max(sa1, axis=0, keepdims=True), jnp.max(sb, axis=0, keepdims=True))

    def soft_diag(h, slot):
        m = mxb[slot][...]
        ta = tb = None
        for c in range(0, hb, CH):
            pa = jnp.exp2((sbuf[slot][c:c + CH, :] - m) * scale2)
            pbuf[slot][c:c + CH, :] = pa.astype(bf)
            part = jnp.sum(pa.reshape(CH // 8, 8, QB), axis=0)
            ta = part if ta is None else ta + part
        for c in range(hb, QB, CH):
            pb = jnp.exp2((sbuf[slot][c:c + CH, hb:] - m[:, hb:]) * scale2)
            pbuf[slot][c:c + CH, hb:] = pb.astype(bf)
            part = jnp.sum(pb.reshape(CH // 8, 8, hb), axis=0)
            tb = part if tb is None else tb + part
        lrow[h, :, :hb] = jnp.sum(ta[:, :hb], axis=0, keepdims=True)
        lrow[h, :, hb:] = jnp.sum(ta[:, hb:] + tb, axis=0, keepdims=True)
        mrow[h] = m

    def weigh_diag(h, slot):
        rows = slice(h * vd, (h + 1) * vd)
        acc[h, :, :hb] = dot_nn(vt[rows, pl.ds(r0, hb)], pbuf[slot][:hb, :hb])
        acc[h, :, hb:] = dot_nn(vt[rows, pl.ds(r0, QB)], pbuf[slot][:, hb:])

    score_diag(0, 0)
    for h in range(GROUP):
        if h + 1 < GROUP:
            score_diag(h + 1, (h + 1) % 2)
        else:
            score(0, 0, 0)
        soft_diag(h, h % 2)
        weigh_diag(h, h % 2)

    def body(kb, _):
        r = pl.multiple_of(kb * QB, QB)
        for h in range(GROUP):
            if h + 1 < GROUP:
                score(h + 1, r, (h + 1) % 2)
            else:
                score(0, pl.multiple_of(r + QB, QB), 0)
            soft(h, h % 2)
            weigh(h, r, h % 2)
        return 0

    lax.fori_loop(0, b, body, 0)

    for h in range(GROUP):
        o_ref[:, h * vd:(h + 1) * vd] = (acc[h] * (1.0 / lrow[h])).T.astype(bf)


def attention_group(g, scale2, kv_rank, nope, rot, vd, kv_all, cq_all, cs_all, wn, wr, uk, uv):
    seq, rank = cq_all.shape
    bf = jnp.bfloat16
    f32 = jnp.float32
    pairs = seq * (seq + QB) // 2
    blocks = seq // QB
    flops = 2 * GROUP * (seq * rank * (nope + rot) + seq * kv_rank * (nope + vd) + pairs * (nope + rot + vd) * 2)
    row = pltpu.VMEM((1, QB), f32)
    return pl.pallas_call(
        functools.partial(attn_kernel, scale2, kv_rank, nope, rot),
        grid=(blocks,),
        in_specs=[
            pl.BlockSpec(kv_all.shape, lambda b: (0, 0)),
            pl.BlockSpec((QB, rank), lambda b: (b, 0)),
            pl.BlockSpec((cs_all.shape[0] // blocks, cs_all.shape[1]), lambda b: (b, 0)),
            pl.BlockSpec((rank, GROUP * nope), lambda b: (0, g)),
            pl.BlockSpec((rank, GROUP * rot), lambda b: (0, g)),
            pl.BlockSpec((kv_rank, GROUP * nope), lambda b: (0, g)),
            pl.BlockSpec((kv_rank, GROUP * vd), lambda b: (0, g)),
        ],
        out_specs=pl.BlockSpec((QB, GROUP * vd), lambda b: (b, 0)),
        out_shape=jax.ShapeDtypeStruct((seq, GROUP * vd), bf),
        scratch_shapes=[
            pltpu.VMEM((GROUP, seq, nope + LANES), bf),
            pltpu.VMEM((GROUP * vd, seq), bf),
            pltpu.VMEM((GROUP * vd, kv_rank), bf),
            pltpu.VMEM((GROUP, QB, nope + LANES), bf),
            pltpu.VMEM((GROUP, vd, QB), f32),
            pltpu.VMEM((GROUP, 1, QB), f32),
            pltpu.VMEM((GROUP, 1, QB), f32),
            pltpu.VMEM((QB, QB), f32),
            pltpu.VMEM((QB, QB), f32),
            pltpu.VMEM((QB, QB), bf),
            pltpu.VMEM((QB, QB), bf),
            row, row, row, row,
        ],
        compiler_params=pltpu.CompilerParams(dimension_semantics=("arbitrary",), vmem_limit_bytes=60_000_000),
        cost_estimate=pl.CostEstimate(flops=flops, bytes_accessed=12_000_000, transcendentals=pairs * GROUP),
        name="mla_attn",
    )(kv_all, cq_all, cs_all, wn, wr, uk, uv)


OSLOTS = 3
NT = 512
NH = 2


def out_kernel(n, call, first, *refs):
    if first:
        o_ref, w_ref, out_ref, wbuf, acc, sem, acc_sem = refs
    else:
        acc_in, o_ref, w_ref, out_ref, wbuf, acc, prev, sem, acc_sem = refs
    rows = o_ref.shape[0] // n
    hidden = w_ref.shape[3]
    wide = hidden // NH
    steps = NH * n

    def copy(s, slot):
        cols = pl.ds(pl.multiple_of(lax.rem(s, NH) * wide, LANES), wide)
        return pltpu.make_async_copy(w_ref.at[s // NH, call, :, cols], wbuf.at[slot], sem.at[slot])

    for s in range(OSLOTS - 1):
        copy(s, s).start()
    if not first:
        pltpu.make_async_copy(acc_in, prev, acc_sem).start()
    acc[...] = jnp.zeros_like(acc)

    def body(s, _):
        slot = lax.rem(s, OSLOTS)

        @pl.when(s + OSLOTS - 1 < steps)
        def _():
            copy(s + OSLOTS - 1, lax.rem(s + OSLOTS - 1, OSLOTS)).start()
        copy(s, slot).wait()
        lhs = o_ref[pl.ds(pl.multiple_of((s // NH) * rows, rows), rows), :]
        side = lax.rem(s, NH)
        for t in range(wide // NT):
            cols = slice(t * NT, (t + 1) * NT)
            acc[side, :, cols] += dot_nn(lhs, wbuf[slot, :, cols])
        return 0

    lax.fori_loop(0, steps, body, 0)
    if first:
        pltpu.make_async_copy(acc, out_ref, acc_sem).start()
        pltpu.make_async_copy(acc, out_ref, acc_sem).wait()
    else:
        pltpu.make_async_copy(acc_in, prev, acc_sem).wait()
        for i in range(NH):
            out_ref[:, i * wide:(i + 1) * wide] = (prev[i] + acc[i]).astype(out_ref.dtype)


def out_product(acc, o, w4, call, n):
    seq, width = o.shape
    rows = seq // n
    hidden = w4.shape[3]
    first = acc is None
    anyspec = pl.BlockSpec(memory_space=pl.ANY)
    vm = pl.BlockSpec(memory_space=pltpu.VMEM)
    args = ([] if first else [acc]) + [o, w4]
    sums = pltpu.VMEM((NH, rows, hidden // NH), jnp.float32)
    return pl.pallas_call(
        functools.partial(out_kernel, n, call, first),
        in_specs=([] if first else [anyspec]) + [vm, anyspec],
        out_specs=anyspec if first else vm,
        out_shape=jax.ShapeDtypeStruct((NH, rows, hidden // NH), jnp.float32) if first else jax.ShapeDtypeStruct((rows, hidden), jnp.bfloat16),
        scratch_shapes=[
            pltpu.VMEM((OSLOTS, width, hidden // NH), jnp.bfloat16),
            sums,
        ] + ([] if first else [sums]) + [
            pltpu.SemaphoreType.DMA((OSLOTS,)),
            pltpu.SemaphoreType.DMA,
        ],
        compiler_params=pltpu.CompilerParams(vmem_limit_bytes=60_000_000),
        cost_estimate=pl.CostEstimate(flops=2 * rows * hidden * width * n, bytes_accessed=2 * hidden * width * n, transcendentals=0),
        name="out_product",
    )(*args)


def solution(mesh):
    n = mesh.shape['sp']
    rows_spec = P(('dp', 'sp'), None)
    tok_spec = P(('dp', 'sp'))
    rep = P()

    def local_step(tok_in, tok_pos, w_dq, g_q, w_uq, w_dkv, g_kv, w_uk, w_uv, w_o):
        num_heads = w_uq.shape[1]
        heads = num_heads // n
        qk_dim = w_uq.shape[2]
        kv_rank = g_kv.shape[0]
        rot = w_dkv.shape[1] - kv_rank
        nope = qk_dim - rot
        vd = w_uv.shape[2]
        scale2 = (0.1 * math.log(YARN_FACTOR) + 1.0) ** 2 / math.sqrt(qk_dim) / math.log(2.0)

        angles = rope_freqs(rot)[:, None] * tok_pos.astype(jnp.float32)[None, :]
        cs_own = jnp.concatenate([jnp.cos(angles), jnp.sin(angles)], axis=0)
        cq_own, cache_kv, cache_pe, kv_own = latents(tok_in, w_dq, w_dkv, g_q, g_kv, cs_own)

        w_t = jnp.transpose(w_uq, (0, 2, 1))
        kv_all, cs_all, cq_all, wn, wr, uk, uv = gather_and_pick(n, heads, nope, kv_own, cs_own, cq_own, w_t, w_uk, w_uv)

        chunks = heads // GROUP
        o_parts = []
        for g in range(chunks):
            o_g = attention_group(g, scale2, kv_rank, nope, rot, vd, kv_all, cq_all, cs_all, wn, wr, uk, uv)
            o_parts.append(lax.all_to_all(o_g, 'sp', 0, 0, tiled=True))
        w4 = w_o.reshape(n, chunks, GROUP * vd, w_o.shape[2])
        acc = None
        for call in range(chunks):
            acc = out_product(acc, o_parts[call], w4, call, n)
        return acc, cache_kv, cache_pe

    return jax.shard_map(local_step, mesh=mesh, in_specs=(rows_spec, tok_spec, rep, rep, rep, rep, rep, rep, rep, rep), out_specs=(rows_spec, rows_spec, rows_spec), check_vma=False)
```

```python
import functools
import math
import jax
import jax.numpy as jnp
from jax import lax
from jax.experimental import pallas as pl
from jax.experimental.pallas import tpu as pltpu
from jax.sharding import PartitionSpec as P

ROPE_THETA = 10000.0
YARN_FACTOR = 40.0
ORIG_CTX = 4096.0
BETA_FAST = 32.0
BETA_SLOW = 1.0
NORM_EPS = 1e-6
MESH = pl.DeviceIdType.MESH
LANES = 128
NEG = -1e30
GROUP = 8


def rope_freqs(rot_dim):
    half_dim = rot_dim // 2
    log_base = 2.0 * math.log(ROPE_THETA)
    low_idx = max(math.floor(rot_dim * math.log(ORIG_CTX / (BETA_FAST * 2.0 * math.pi)) / log_base), 0)
    high_idx = min(math.ceil(rot_dim * math.log(ORIG_CTX / (BETA_SLOW * 2.0 * math.pi)) / log_base), half_dim - 1)
    spread = max(high_idx - low_idx, 0.001)
    freq_list = []
    for freq_idx in range(half_dim):
        base_freq = ROPE_THETA ** (-2.0 * freq_idx / rot_dim)
        ramp_val = min(max((freq_idx - low_idx) / spread, 0.0), 1.0)
        freq_list.append(base_freq / YARN_FACTOR * ramp_val + base_freq * (1.0 - ramp_val))
    return jnp.asarray(freq_list, dtype=jnp.float32)


def rotate_half(act_in, cos_t, sin_t):
    half_dim = act_in.shape[-1] // 2
    first = act_in[..., :half_dim]
    second = act_in[..., half_dim:]
    return jnp.concatenate([first * cos_t - second * sin_t, second * cos_t + first * sin_t], axis=-1)


def rms_norm(act_in, gain):
    mean_sq = jnp.mean(act_in * act_in, axis=-1, keepdims=True)
    return act_in * lax.rsqrt(mean_sq + NORM_EPS) * gain


def dot_nt(a, b):
    return lax.dot_general(a, b, (((1,), (1,)), ((), ())), preferred_element_type=jnp.float32)


def dot_nn(a, b):
    return jnp.dot(a, b, preferred_element_type=jnp.float32)


LK = 1024
LSLOTS = 4


def latent_kernel(kv_rank, x_ref, wq_ref, wkvt_ref, gq_ref, gkv_ref, cs_ref, cq_ref, kv_ref, pe_ref, own_ref, xb, qb, kb, acc_q, acc_kv, sem):
    bf = jnp.bfloat16
    steps = x_ref.shape[1] // LK

    def copies(s, slot):
        k = pl.ds(pl.multiple_of(s * LK, LK), LK)
        return (
            pltpu.make_async_copy(x_ref.at[:, k], xb.at[slot], sem.at[0, slot]),
            pltpu.make_async_copy(wq_ref.at[k, :], qb.at[slot], sem.at[1, slot]),
            pltpu.make_async_copy(wkvt_ref.at[:, k], kb.at[slot], sem.at[2, slot]),
        )

    for s in range(LSLOTS - 1):
        for c in copies(s, s):
            c.start()
    acc_q[...] = jnp.zeros_like(acc_q)
    acc_kv[...] = jnp.zeros_like(acc_kv)

    def body(s, _):
        slot = lax.rem(s, LSLOTS)

        @pl.when(s + LSLOTS - 1 < steps)
        def _():
            for c in copies(s + LSLOTS - 1, lax.rem(s + LSLOTS - 1, LSLOTS)):
                c.start()
        for c in copies(s, slot):
            c.wait()
        x = xb[slot]
        acc_q[...] += dot_nn(x, qb[slot])
        acc_kv[...] += dot_nt(x, kb[slot])
        return 0

    lax.fori_loop(0, steps, body, 0)
    cq_ref[...] = rms_norm(acc_q[...], gq_ref[...].reshape(1, -1)).astype(bf)
    lat = rms_norm(acc_kv[:, :kv_rank], gkv_ref[...].reshape(1, -1)).astype(bf)
    kv_ref[...] = lat
    cs = cs_ref[...].T
    half = cs.shape[1] // 2
    pe = rotate_half(acc_kv[:, kv_rank:], cs[:, :half], cs[:, half:]).astype(bf)
    pe_ref[...] = pe
    own_ref[:, :kv_rank] = lat
    own_ref[:, kv_rank:] = jnp.concatenate([pe, jnp.zeros((pe.shape[0], LANES - pe.shape[1]), bf)], axis=1)


def latents(x, w_dq, w_dkv, g_q, g_kv, cs_own):
    rows, hidden = x.shape
    rank = w_dq.shape[1]
    kvw = w_dkv.shape[1]
    kv_rank = g_kv.shape[0]
    rot = kvw - kv_rank
    bf = jnp.bfloat16
    anyspec = pl.BlockSpec(memory_space=pl.ANY)
    vm = pl.BlockSpec(memory_space=pltpu.VMEM)
    return pl.pallas_call(
        functools.partial(latent_kernel, kv_rank),
        in_specs=[anyspec] * 3 + [vm] * 3,
        out_specs=[vm] * 4,
        out_shape=[
            jax.ShapeDtypeStruct((rows, rank), bf),
            jax.ShapeDtypeStruct((rows, kv_rank), bf),
            jax.ShapeDtypeStruct((rows, rot), bf),
            jax.ShapeDtypeStruct((rows, kv_rank + LANES), bf),
        ],
        scratch_shapes=[
            pltpu.VMEM((LSLOTS, rows, LK), bf),
            pltpu.VMEM((LSLOTS, LK, rank), bf),
            pltpu.VMEM((LSLOTS, kvw, LK), bf),
            pltpu.VMEM((rows, rank), jnp.float32),
            pltpu.VMEM((rows, kvw), jnp.float32),
            pltpu.SemaphoreType.DMA((3, LSLOTS)),
        ],
        compiler_params=pltpu.CompilerParams(vmem_limit_bytes=60_000_000),
        cost_estimate=pl.CostEstimate(flops=2 * rows * hidden * (rank + kvw), bytes_accessed=2 * hidden * (rank + kvw + rows), transcendentals=0),
        name="latents",
    )(x, w_dq, w_dkv.T, g_q, g_kv, cs_own)


SUB = 16
CBLK = 96


def gather_kernel(n, heads, nope, kv_ref, cs_ref, cq_ref, wt_ref, uk_ref, uv_ref, kv_all, cs_all, cq_all, wn_ref, wr_ref, uko_ref, uvo_ref, sel, tn, tr, tu, send_sem, recv_sem, loc_sem):
    step = pl.program_id(0)
    last = pl.num_programs(0) - 1
    me = lax.axis_index("sp")
    right = lax.rem(me + 2, n)
    left = lax.rem(me + n - 2, n)
    mate = me + 1 - 2 * lax.rem(me, 2)
    opp = lax.rem(me + 4, n)
    srcs = (kv_ref, cs_ref, cq_ref)
    alls = (kv_all, cs_all, cq_all)
    num = len(srcs)
    bf = jnp.bfloat16

    def piece(arr, owner, part):
        rows = srcs[arr].shape[0]
        half = rows // 2
        off, size = ((0, half), (half, half), (0, rows))[part]
        return alls[arr].at[pl.ds(pl.multiple_of(owner * rows + off, half), size)]

    def own(arr, part):
        half = srcs[arr].shape[0] // 2
        return srcs[arr].at[pl.ds(0, half)] if part == 0 else srcs[arr].at[pl.ds(half, half)] if part == 1 else srcs[arr]

    def rcopy(arr, idx, src, owner, part, dev):
        return pltpu.make_async_remote_copy(
            src_ref=src, dst_ref=piece(arr, owner, part),
            send_sem=send_sem.at[arr, idx], recv_sem=recv_sem.at[arr, idx],
            device_id={"sp": dev}, device_id_type=MESH)

    def copies(arr):
        return [
            rcopy(arr, 0, own(arr, 0), me, 0, right),
            rcopy(arr, 1, own(arr, 1), me, 1, right),
            rcopy(arr, 2, own(arr, 1), me, 1, left),
            rcopy(arr, 3, own(arr, 0), me, 0, left),
            rcopy(arr, 4, own(arr, 2), me, 2, mate),
            rcopy(arr, 5, piece(arr, left, 0), left, 0, right),
            rcopy(arr, 6, piece(arr, right, 1), right, 1, left),
            rcopy(arr, 7, piece(arr, left, 2), left, 2, mate),
            rcopy(arr, 8, piece(arr, right, 2), right, 2, mate),
            rcopy(arr, 9, piece(arr, opp, 0), opp, 0, mate),
            rcopy(arr, 10, piece(arr, opp, 1), opp, 1, mate),
        ]

    cps = [copies(arr) for arr in range(num)]
    loc = [pltpu.make_async_copy(srcs[arr], piece(arr, me, 2), loc_sem.at[arr]) for arr in range(num)]
    width = SUB * heads // 2
    pairs = heads // 2
    lanes = wt_ref.shape[2]

    @pl.when(step == 0)
    def _():
        barrier = pltpu.get_barrier_semaphore()
        for dev in (left, right, mate):
            pl.semaphore_signal(barrier, inc=1, device_id={"sp": dev}, device_id_type=MESH)
        pl.semaphore_wait(barrier, 3)
        for arr in (2, 0, 1):
            for i in (0, 2, 1, 3, 4):
                cps[arr][i].start()
        for arr in range(num):
            loc[arr].start()
        hp = lax.broadcasted_iota(jnp.int32, (lanes, 2 * width), 0)
        col = lax.broadcasted_iota(jnp.int32, (lanes, 2 * width), 1)
        want_h = me * heads + 2 * lax.rem(col, pairs) + col // width
        want_c = lax.rem(col, width) // pairs
        code = jnp.where(hp == want_h, want_c, -1)
        for c in range(SUB):
            sel[c * lanes:(c + 1) * lanes, :] = jnp.where(code == c, 1.0, 0.0).astype(bf)

    def hand_on(arr):
        cps[arr][0].wait_recv()
        cps[arr][5].start()
        cps[arr][2].wait_recv()
        cps[arr][6].start()

    def to_mate(arr):
        cps[arr][1].wait_recv()
        cps[arr][7].start()
        cps[arr][3].wait_recv()
        cps[arr][8].start()

    @pl.when(step == (5 * last) // 15)
    def _():
        hand_on(2)

    @pl.when(step == (8 * last) // 15)
    def _():
        to_mate(2)

    @pl.when(step == (10 * last) // 15)
    def _():
        hand_on(0)

    @pl.when(step == (12 * last) // 15)
    def _():
        hand_on(1)
        to_mate(0)

    for s in range(CBLK // SUB):
        lhs = jnp.concatenate([wt_ref[s * SUB + i] for i in range(SUB)], axis=1)
        g = dot_nn(lhs, sel[...])
        tn[s] = g[:nope].T
        tr[s] = jnp.concatenate([g[nope:, :width], g[nope:, width:]], axis=0).T
        for h in range(heads):
            par, hp = h % 2, h // 2
            wn_ref[s * SUB:(s + 1) * SUB, h * nope:(h + 1) * nope] = tn[s, pl.ds(par * width + hp, SUB, stride=pairs), :].astype(bf)
        for hp in range(pairs):
            wr_ref[s * SUB:(s + 1) * SUB, hp * LANES:(hp + 1) * LANES] = tr[s, pl.ds(hp, SUB, stride=pairs), :].astype(bf)

    cb = uk_ref.shape[0]
    for i, (src, dst) in enumerate(((uk_ref, uko_ref), (uv_ref, uvo_ref))):
        wd = src.shape[2]
        tu[i] = src[...].astype(jnp.float32).reshape(cb * heads, wd)
        for h in range(heads):
            dst[:, h * wd:(h + 1) * wd] = tu[i, pl.ds(h, cb, stride=heads), :].astype(bf)

    @pl.when(step == last)
    def _():
        to_mate(1)
        for arr in (2, 0, 1):
            cps[arr][5].wait_recv()
            cps[arr][9].start()
            cps[arr][6].wait_recv()
            cps[arr][10].start()
        for arr in range(num):
            for i in (4, 7, 8, 9, 10):
                cps[arr][i].wait_recv()
            for i in range(11):
                cps[arr][i].wait_send()
            loc[arr].wait()


def gather_and_pick(n, heads, nope, kv_own, cs_own, cq_own, w_t, w_uk, w_uv):
    rank = cq_own.shape[1]
    qk = w_t.shape[1]
    kv_rank = w_uk.shape[0]
    vd = w_uv.shape[2]
    steps = rank // CBLK
    cb = kv_rank // steps
    bf = jnp.bfloat16
    f32 = jnp.float32
    const = lambda s: (0, 0)
    own_heads = lambda s: (s, lax.axis_index("sp"), 0)
    return pl.pallas_call(
        functools.partial(gather_kernel, n, heads, nope),
        grid=(steps,),
        in_specs=[
            pl.BlockSpec(kv_own.shape, const),
            pl.BlockSpec(cs_own.shape, const),
            pl.BlockSpec(cq_own.shape, const),
            pl.BlockSpec((CBLK, qk, w_t.shape[2]), lambda s: (s, 0, 0)),
            pl.BlockSpec((cb, heads, nope), own_heads),
            pl.BlockSpec((cb, heads, vd), own_heads),
        ],
        out_specs=[
            pl.BlockSpec(memory_space=pl.ANY),
            pl.BlockSpec(memory_space=pl.ANY),
            pl.BlockSpec(memory_space=pl.ANY),
            pl.BlockSpec((CBLK, heads * nope), lambda s: (s, 0)),
            pl.BlockSpec((CBLK, heads * (qk - nope)), lambda s: (s, 0)),
            pl.BlockSpec((cb, heads * nope), lambda s: (s, 0)),
            pl.BlockSpec((cb, heads * vd), lambda s: (s, 0)),
        ],
        out_shape=[
            jax.ShapeDtypeStruct((n * kv_own.shape[0], kv_own.shape[1]), bf),
            jax.ShapeDtypeStruct((n * cs_own.shape[0], cs_own.shape[1]), f32),
            jax.ShapeDtypeStruct((n * cq_own.shape[0], rank), bf),
            jax.ShapeDtypeStruct((rank, heads * nope), bf),
            jax.ShapeDtypeStruct((rank, heads * (qk - nope)), bf),
            jax.ShapeDtypeStruct((kv_rank, heads * nope), bf),
            jax.ShapeDtypeStruct((kv_rank, heads * vd), bf),
        ],
        scratch_shapes=[
            pltpu.VMEM((SUB * w_t.shape[2], SUB * heads), bf),
            pltpu.VMEM((CBLK // SUB, SUB * heads, nope), f32),
            pltpu.VMEM((CBLK // SUB, SUB * heads // 2, LANES), f32),
            pltpu.VMEM((2, cb * heads, nope), f32),
            pltpu.SemaphoreType.DMA((3, 11)),
            pltpu.SemaphoreType.DMA((3, 11)),
            pltpu.SemaphoreType.DMA((3,)),
        ],
        compiler_params=pltpu.CompilerParams(collective_id=0, has_side_effects=True, dimension_semantics=("arbitrary",), vmem_limit_bytes=60_000_000),
        cost_estimate=pl.CostEstimate(flops=30_000_000_000, bytes_accessed=90_000_000, transcendentals=0),
        name="gather_pick",
    )(kv_own, cs_own, cq_own, w_t, w_uk, w_uv)


QB = 512
CH = 16


def attn_kernel(g, scale2, kv_rank, nope, rot, kv_ref, cq_ref, cs_ref, wn_hbm, wr_hbm, uk_ref, uv_ref, o_ref, wn_ref, wr_ref, wsem, kcat, vt, uvt, qcat, acc, mrow, lrow, s0, s1, p0, p1, mx0, mx1, al0, al1):
    b = pl.program_id(0)
    vd = uv_ref.shape[1] // GROUP
    bf = jnp.bfloat16
    sbuf, pbuf, mxb, alb = (s0, s1), (p0, p1), (mx0, mx1), (al0, al1)
    hd = rot // 2
    hb = QB // 2

    @pl.when(b == 0)
    def _():
        loads = [
            pltpu.make_async_copy(src.at[:, pl.ds(g * dst.shape[1], dst.shape[1])], dst, wsem.at[i])
            for i, (src, dst) in enumerate(((wn_hbm, wn_ref), (wr_hbm, wr_ref)))
        ]
        for c in loads:
            c.start()
        uvt[...] = uv_ref[...].T

        def fill(i, _):
            r = pl.ds(pl.multiple_of(i * QB, QB), QB)
            c = kv_ref[r, :kv_rank]
            k = dot_nn(c, uk_ref[...]).astype(bf)
            pe_f = kv_ref[r, kv_rank:kv_rank + LANES].astype(jnp.float32)
            pe = (pe_f.astype(bf), pltpu.roll(pe_f, rot, 1).astype(bf))
            for h in range(GROUP):
                kcat[h, r, :nope] = k[:, h * nope:(h + 1) * nope]
                kcat[h, r, nope:] = pe[h % 2]
            vt[:, r] = dot_nt(uvt[...], c).astype(bf)
            return 0
        lax.fori_loop(0, kv_ref.shape[0] // QB, fill, 0)
        for c in loads:
            c.wait()

    cq = cq_ref[...]
    qn = dot_nn(cq, wn_ref[...]).astype(bf)
    qr = dot_nn(cq, wr_ref[...])
    per = cs_ref.shape[1]
    cos_p, sin_p = [], []
    for j in range(QB // per):
        c_t = cs_ref[j * rot:j * rot + hd, :]
        s_t = cs_ref[j * rot + hd:(j + 1) * rot, :]
        cos_p.append(jnp.concatenate([c_t] * (LANES // hd), axis=0).T)
        sin_p.append(jnp.concatenate([-s_t, s_t] * (LANES // rot), axis=0).T)
    cos_t = jnp.concatenate(cos_p, axis=0)
    sin_t = jnp.concatenate(sin_p, axis=0)
    for pr in range(GROUP // 2):
        z = qr[:, pr * LANES:(pr + 1) * LANES]
        lane = lax.broadcasted_iota(jnp.int32, z.shape, 1)
        swapped = jnp.where((lane // hd) % 2 == 0, pltpu.roll(z, LANES - hd, 1), pltpu.roll(z, hd, 1))
        zr = (z * cos_t + swapped * sin_t).astype(bf)
        for m in range(2):
            h = 2 * pr + m
            qcat[h, :, :nope] = qn[:, h * nope:(h + 1) * nope]
            qcat[h, :, nope:] = zr

    r0 = pl.multiple_of(b * QB, QB)
    tri = lax.broadcasted_iota(jnp.int32, (hb, hb), 0) <= lax.broadcasted_iota(jnp.int32, (hb, hb), 1)

    def score(h, r, slot):
        m = None
        for c in (0, hb):
            s = dot_nt(kcat[h, pl.ds(r + c, hb), :], qcat[h])
            sbuf[slot][c:c + hb, :] = s
            mc = jnp.max(s, axis=0, keepdims=True)
            m = mc if m is None else jnp.maximum(m, mc)
        mxb[slot][...] = m

    def soft(h, slot):
        m_old = mrow[h]
        m_new = jnp.maximum(m_old, mxb[slot][...])
        alpha = jnp.exp2((m_old - m_new) * scale2)
        tot = None
        for c in range(0, QB, CH):
            p = jnp.exp2((sbuf[slot][c:c + CH, :] - m_new) * scale2)
            pbuf[slot][c:c + CH, :] = p.astype(bf)
            part = jnp.sum(p.reshape(CH // 8, 8, QB), axis=0)
            tot = part if tot is None else tot + part
        lrow[h] = lrow[h] * alpha + jnp.sum(tot, axis=0, keepdims=True)
        mrow[h] = m_new
        alb[slot][...] = alpha

    def weigh(h, r, slot):
        v = vt[h * vd:(h + 1) * vd, pl.ds(r, QB)]
        acc[h] = acc[h] * alb[slot][...] + dot_nn(v, pbuf[slot][...])

    def score_diag(h, slot):
        k = kcat[h, pl.ds(r0, QB), :]
        q = qcat[h]
        sa = dot_nt(k[:hb], q)
        sa0 = jnp.where(tri, sa[:, :hb], NEG)
        sa1 = sa[:, hb:]
        sb = jnp.where(tri, dot_nt(k[hb:], q[hb:]), NEG)
        sbuf[slot][:hb, :hb] = sa0
        sbuf[slot][:hb, hb:] = sa1
        sbuf[slot][hb:, hb:] = sb
        mxb[slot][:, :hb] = jnp.max(sa0, axis=0, keepdims=True)
        mxb[slot][:, hb:] = jnp.maximum(jnp.max(sa1, axis=0, keepdims=True), jnp.max(sb, axis=0, keepdims=True))

    def soft_diag(h, slot):
        m = mxb[slot][...]
        ta = tb = None
        for c in range(0, hb, CH):
            pa = jnp.exp2((sbuf[slot][c:c + CH, :] - m) * scale2)
            pbuf[slot][c:c + CH, :] = pa.astype(bf)
            part = jnp.sum(pa.reshape(CH // 8, 8, QB), axis=0)
            ta = part if ta is None else ta + part
        for c in range(hb, QB, CH):
            pb = jnp.exp2((sbuf[slot][c:c + CH, hb:] - m[:, hb:]) * scale2)
            pbuf[slot][c:c + CH, hb:] = pb.astype(bf)
            part = jnp.sum(pb.reshape(CH // 8, 8, hb), axis=0)
            tb = part if tb is None else tb + part
        lrow[h, :, :hb] = jnp.sum(ta[:, :hb], axis=0, keepdims=True)
        lrow[h, :, hb:] = jnp.sum(ta[:, hb:] + tb, axis=0, keepdims=True)
        mrow[h] = m

    def weigh_diag(h, slot):
        rows = slice(h * vd, (h + 1) * vd)
        acc[h, :, :hb] = dot_nn(vt[rows, pl.ds(r0, hb)], pbuf[slot][:hb, :hb])
        acc[h, :, hb:] = dot_nn(vt[rows, pl.ds(r0, QB)], pbuf[slot][:, hb:])

    score_diag(0, 0)
    for h in range(GROUP):
        if h + 1 < GROUP:
            score_diag(h + 1, (h + 1) % 2)
        else:
            score(0, 0, 0)
        soft_diag(h, h % 2)
        weigh_diag(h, h % 2)

    def body(kb, _):
        r = pl.multiple_of(kb * QB, QB)
        for h in range(GROUP):
            if h + 1 < GROUP:
                score(h + 1, r, (h + 1) % 2)
            else:
                score(0, pl.multiple_of(r + QB, QB), 0)
            soft(h, h % 2)
            weigh(h, r, h % 2)
        return 0

    lax.fori_loop(0, b, body, 0)

    for h in range(GROUP):
        o_ref[:, h * vd:(h + 1) * vd] = (acc[h] * (1.0 / lrow[h])).T.astype(bf)


def attention_group(g, scale2, kv_rank, nope, rot, vd, kv_all, cq_all, cs_all, wn, wr, uk, uv):
    seq, rank = cq_all.shape
    bf = jnp.bfloat16
    f32 = jnp.float32
    pairs = seq * (seq + QB) // 2
    blocks = seq // QB
    flops = 2 * GROUP * (seq * rank * (nope + rot) + seq * kv_rank * (nope + vd) + pairs * (nope + rot + vd) * 2)
    row = pltpu.VMEM((1, QB), f32)
    return pl.pallas_call(
        functools.partial(attn_kernel, g, scale2, kv_rank, nope, rot),
        grid=(blocks,),
        in_specs=[
            pl.BlockSpec(kv_all.shape, lambda b: (0, 0)),
            pl.BlockSpec((QB, rank), lambda b: (b, 0)),
            pl.BlockSpec((cs_all.shape[0] // blocks, cs_all.shape[1]), lambda b: (b, 0)),
            pl.BlockSpec(memory_space=pl.ANY),
            pl.BlockSpec(memory_space=pl.ANY),
            pl.BlockSpec((kv_rank, GROUP * nope), lambda b: (0, g)),
            pl.BlockSpec((kv_rank, GROUP * vd), lambda b: (0, g)),
        ],
        out_specs=pl.BlockSpec((QB, GROUP * vd), lambda b: (b, 0)),
        out_shape=jax.ShapeDtypeStruct((seq, GROUP * vd), bf),
        scratch_shapes=[
            pltpu.VMEM((rank, GROUP * nope), bf),
            pltpu.VMEM((rank, GROUP * rot), bf),
            pltpu.SemaphoreType.DMA((2,)),
            pltpu.VMEM((GROUP, seq, nope + LANES), bf),
            pltpu.VMEM((GROUP * vd, seq), bf),
            pltpu.VMEM((GROUP * vd, kv_rank), bf),
            pltpu.VMEM((GROUP, QB, nope + LANES), bf),
            pltpu.VMEM((GROUP, vd, QB), f32),
            pltpu.VMEM((GROUP, 1, QB), f32),
            pltpu.VMEM((GROUP, 1, QB), f32),
            pltpu.VMEM((QB, QB), f32),
            pltpu.VMEM((QB, QB), f32),
            pltpu.VMEM((QB, QB), bf),
            pltpu.VMEM((QB, QB), bf),
            row, row, row, row,
        ],
        compiler_params=pltpu.CompilerParams(dimension_semantics=("arbitrary",), vmem_limit_bytes=60_000_000),
        cost_estimate=pl.CostEstimate(flops=flops, bytes_accessed=12_000_000, transcendentals=pairs * GROUP),
        name="mla_attn",
    )(kv_all, cq_all, cs_all, wn, wr, uk, uv)


OSLOTS = 3
NT = 512
NH = 2


def out_kernel(n, call, first, *refs):
    if first:
        o_ref, w_ref, out_ref, wbuf, acc, sem, acc_sem = refs
    else:
        acc_in, o_ref, w_ref, out_ref, wbuf, acc, prev, sem, acc_sem = refs
    rows = o_ref.shape[0] // n
    hidden = w_ref.shape[3]
    wide = hidden // NH
    steps = NH * n

    def copy(s, slot):
        cols = pl.ds(pl.multiple_of(lax.rem(s, NH) * wide, LANES), wide)
        return pltpu.make_async_copy(w_ref.at[s // NH, call, :, cols], wbuf.at[slot], sem.at[slot])

    for s in range(OSLOTS - 1):
        copy(s, s).start()
    if not first:
        pltpu.make_async_copy(acc_in, prev, acc_sem).start()
    acc[...] = jnp.zeros_like(acc)

    def body(s, _):
        slot = lax.rem(s, OSLOTS)

        @pl.when(s + OSLOTS - 1 < steps)
        def _():
            copy(s + OSLOTS - 1, lax.rem(s + OSLOTS - 1, OSLOTS)).start()
        copy(s, slot).wait()
        lhs = o_ref[pl.ds(pl.multiple_of((s // NH) * rows, rows), rows), :]
        side = lax.rem(s, NH)
        for t in range(wide // NT):
            cols = slice(t * NT, (t + 1) * NT)
            acc[side, :, cols] += dot_nn(lhs, wbuf[slot, :, cols])
        return 0

    lax.fori_loop(0, steps, body, 0)
    if first:
        pltpu.make_async_copy(acc, out_ref, acc_sem).start()
        pltpu.make_async_copy(acc, out_ref, acc_sem).wait()
    else:
        pltpu.make_async_copy(acc_in, prev, acc_sem).wait()
        for i in range(NH):
            out_ref[:, i * wide:(i + 1) * wide] = (prev[i] + acc[i]).astype(out_ref.dtype)


def out_product(acc, o, w4, call, n):
    seq, width = o.shape
    rows = seq // n
    hidden = w4.shape[3]
    first = acc is None
    anyspec = pl.BlockSpec(memory_space=pl.ANY)
    vm = pl.BlockSpec(memory_space=pltpu.VMEM)
    args = ([] if first else [acc]) + [o, w4]
    sums = pltpu.VMEM((NH, rows, hidden // NH), jnp.float32)
    return pl.pallas_call(
        functools.partial(out_kernel, n, call, first),
        in_specs=([] if first else [anyspec]) + [vm, anyspec],
        out_specs=anyspec if first else vm,
        out_shape=jax.ShapeDtypeStruct((NH, rows, hidden // NH), jnp.float32) if first else jax.ShapeDtypeStruct((rows, hidden), jnp.bfloat16),
        scratch_shapes=[
            pltpu.VMEM((OSLOTS, width, hidden // NH), jnp.bfloat16),
            sums,
        ] + ([] if first else [sums]) + [
            pltpu.SemaphoreType.DMA((OSLOTS,)),
            pltpu.SemaphoreType.DMA,
        ],
        compiler_params=pltpu.CompilerParams(vmem_limit_bytes=60_000_000),
        cost_estimate=pl.CostEstimate(flops=2 * rows * hidden * width * n, bytes_accessed=2 * hidden * width * n, transcendentals=0),
        name="out_product",
    )(*args)


def solution(mesh):
    n = mesh.shape['sp']
    rows_spec = P(('dp', 'sp'), None)
    tok_spec = P(('dp', 'sp'))
    rep = P()

    def local_step(tok_in, tok_pos, w_dq, g_q, w_uq, w_dkv, g_kv, w_uk, w_uv, w_o):
        num_heads = w_uq.shape[1]
        heads = num_heads // n
        qk_dim = w_uq.shape[2]
        kv_rank = g_kv.shape[0]
        rot = w_dkv.shape[1] - kv_rank
        nope = qk_dim - rot
        vd = w_uv.shape[2]
        scale2 = (0.1 * math.log(YARN_FACTOR) + 1.0) ** 2 / math.sqrt(qk_dim) / math.log(2.0)

        angles = rope_freqs(rot)[:, None] * tok_pos.astype(jnp.float32)[None, :]
        cs_own = jnp.concatenate([jnp.cos(angles), jnp.sin(angles)], axis=0)
        cq_own, cache_kv, cache_pe, kv_own = latents(tok_in, w_dq, w_dkv, g_q, g_kv, cs_own)

        w_t = jnp.transpose(w_uq, (0, 2, 1))
        kv_all, cs_all, cq_all, wn, wr, uk, uv = gather_and_pick(n, heads, nope, kv_own, cs_own, cq_own, w_t, w_uk, w_uv)

        chunks = heads // GROUP
        o_parts = []
        for g in range(chunks):
            o_g = attention_group(g, scale2, kv_rank, nope, rot, vd, kv_all, cq_all, cs_all, wn, wr, uk, uv)
            o_parts.append(lax.all_to_all(o_g, 'sp', 0, 0, tiled=True))
        w4 = w_o.reshape(n, chunks, GROUP * vd, w_o.shape[2])
        acc = None
        for call in range(chunks):
            acc = out_product(acc, o_parts[call], w4, call, n)
        return acc, cache_kv, cache_pe

    return jax.shard_map(local_step, mesh=mesh, in_specs=(rows_spec, tok_spec, rep, rep, rep, rep, rep, rep, rep, rep), out_specs=(rows_spec, rows_spec, rows_spec), check_vma=False)
```

```python
import functools
import math
import jax
import jax.numpy as jnp
from jax import lax
from jax.experimental import pallas as pl
from jax.experimental.pallas import tpu as pltpu
from jax.sharding import PartitionSpec as P

ROPE_THETA = 10000.0
YARN_FACTOR = 40.0
ORIG_CTX = 4096.0
BETA_FAST = 32.0
BETA_SLOW = 1.0
NORM_EPS = 1e-6
MESH = pl.DeviceIdType.MESH
LANES = 128
NEG = -1e30
GROUP = 8


def rope_freqs(rot_dim):
    half_dim = rot_dim // 2
    log_base = 2.0 * math.log(ROPE_THETA)
    low_idx = max(math.floor(rot_dim * math.log(ORIG_CTX / (BETA_FAST * 2.0 * math.pi)) / log_base), 0)
    high_idx = min(math.ceil(rot_dim * math.log(ORIG_CTX / (BETA_SLOW * 2.0 * math.pi)) / log_base), half_dim - 1)
    spread = max(high_idx - low_idx, 0.001)
    freq_list = []
    for freq_idx in range(half_dim):
        base_freq = ROPE_THETA ** (-2.0 * freq_idx / rot_dim)
        ramp_val = min(max((freq_idx - low_idx) / spread, 0.0), 1.0)
        freq_list.append(base_freq / YARN_FACTOR * ramp_val + base_freq * (1.0 - ramp_val))
    return jnp.asarray(freq_list, dtype=jnp.float32)


def rotate_half(act_in, cos_t, sin_t):
    half_dim = act_in.shape[-1] // 2
    first = act_in[..., :half_dim]
    second = act_in[..., half_dim:]
    return jnp.concatenate([first * cos_t - second * sin_t, second * cos_t + first * sin_t], axis=-1)


def rms_norm(act_in, gain):
    mean_sq = jnp.mean(act_in * act_in, axis=-1, keepdims=True)
    return act_in * lax.rsqrt(mean_sq + NORM_EPS) * gain


def dot_nt(a, b):
    return lax.dot_general(a, b, (((1,), (1,)), ((), ())), preferred_element_type=jnp.float32)


def dot_nn(a, b):
    return jnp.dot(a, b, preferred_element_type=jnp.float32)


LK = 1024
LSLOTS = 4


def latent_kernel(kv_rank, x_ref, wq_ref, wkvt_ref, gq_ref, gkv_ref, cs_ref, cq_ref, kv_ref, pe_ref, own_ref, xb, qb, kb, acc_q, acc_kv, sem):
    bf = jnp.bfloat16
    steps = x_ref.shape[1] // LK

    def copies(s, slot):
        k = pl.ds(pl.multiple_of(s * LK, LK), LK)
        return (
            pltpu.make_async_copy(x_ref.at[:, k], xb.at[slot], sem.at[0, slot]),
            pltpu.make_async_copy(wq_ref.at[k, :], qb.at[slot], sem.at[1, slot]),
            pltpu.make_async_copy(wkvt_ref.at[:, k], kb.at[slot], sem.at[2, slot]),
        )

    for s in range(LSLOTS - 1):
        for c in copies(s, s):
            c.start()
    acc_q[...] = jnp.zeros_like(acc_q)
    acc_kv[...] = jnp.zeros_like(acc_kv)

    def body(s, _):
        slot = lax.rem(s, LSLOTS)

        @pl.when(s + LSLOTS - 1 < steps)
        def _():
            for c in copies(s + LSLOTS - 1, lax.rem(s + LSLOTS - 1, LSLOTS)):
                c.start()
        for c in copies(s, slot):
            c.wait()
        x = xb[slot]
        acc_q[...] += dot_nn(x, qb[slot])
        acc_kv[...] += dot_nt(x, kb[slot])
        return 0

    lax.fori_loop(0, steps, body, 0)
    cq_ref[...] = rms_norm(acc_q[...], gq_ref[...].reshape(1, -1)).astype(bf)
    lat = rms_norm(acc_kv[:, :kv_rank], gkv_ref[...].reshape(1, -1)).astype(bf)
    kv_ref[...] = lat
    cs = cs_ref[...].T
    half = cs.shape[1] // 2
    pe = rotate_half(acc_kv[:, kv_rank:], cs[:, :half], cs[:, half:]).astype(bf)
    pe_ref[...] = pe
    own_ref[:, :kv_rank] = lat
    own_ref[:, kv_rank:] = jnp.concatenate([pe, jnp.zeros((pe.shape[0], LANES - pe.shape[1]), bf)], axis=1)


def latents(x, w_dq, w_dkv, g_q, g_kv, cs_own):
    rows, hidden = x.shape
    rank = w_dq.shape[1]
    kvw = w_dkv.shape[1]
    kv_rank = g_kv.shape[0]
    rot = kvw - kv_rank
    bf = jnp.bfloat16
    anyspec = pl.BlockSpec(memory_space=pl.ANY)
    vm = pl.BlockSpec(memory_space=pltpu.VMEM)
    return pl.pallas_call(
        functools.partial(latent_kernel, kv_rank),
        in_specs=[anyspec] * 3 + [vm] * 3,
        out_specs=[vm] * 4,
        out_shape=[
            jax.ShapeDtypeStruct((rows, rank), bf),
            jax.ShapeDtypeStruct((rows, kv_rank), bf),
            jax.ShapeDtypeStruct((rows, rot), bf),
            jax.ShapeDtypeStruct((rows, kv_rank + LANES), bf),
        ],
        scratch_shapes=[
            pltpu.VMEM((LSLOTS, rows, LK), bf),
            pltpu.VMEM((LSLOTS, LK, rank), bf),
            pltpu.VMEM((LSLOTS, kvw, LK), bf),
            pltpu.VMEM((rows, rank), jnp.float32),
            pltpu.VMEM((rows, kvw), jnp.float32),
            pltpu.SemaphoreType.DMA((3, LSLOTS)),
        ],
        compiler_params=pltpu.CompilerParams(vmem_limit_bytes=60_000_000),
        cost_estimate=pl.CostEstimate(flops=2 * rows * hidden * (rank + kvw), bytes_accessed=2 * hidden * (rank + kvw + rows), transcendentals=0),
        name="latents",
    )(x, w_dq, w_dkv.T, g_q, g_kv, cs_own)


SUB = 16
CBLK = 96


def gather_kernel(n, heads, nope, kv_ref, cs_ref, cq_ref, wt_ref, uk_ref, uv_ref, kv_all, cs_all, cq_all, wn_ref, wr_ref, uko_ref, uvo_ref, sel, tn, tr, tu, send_sem, recv_sem, loc_sem):
    step = pl.program_id(0)
    last = pl.num_programs(0) - 1
    me = lax.axis_index("sp")
    right = lax.rem(me + 2, n)
    left = lax.rem(me + n - 2, n)
    mate = me + 1 - 2 * lax.rem(me, 2)
    opp = lax.rem(me + 4, n)
    srcs = (kv_ref, cs_ref, cq_ref)
    alls = (kv_all, cs_all, cq_all)
    num = len(srcs)
    bf = jnp.bfloat16

    def piece(arr, owner, part):
        rows = srcs[arr].shape[0]
        half = rows // 2
        off, size = ((0, half), (half, half), (0, rows))[part]
        return alls[arr].at[pl.ds(pl.multiple_of(owner * rows + off, half), size)]

    def own(arr, part):
        half = srcs[arr].shape[0] // 2
        return srcs[arr].at[pl.ds(0, half)] if part == 0 else srcs[arr].at[pl.ds(half, half)] if part == 1 else srcs[arr]

    def rcopy(arr, idx, src, owner, part, dev):
        return pltpu.make_async_remote_copy(
            src_ref=src, dst_ref=piece(arr, owner, part),
            send_sem=send_sem.at[arr, idx], recv_sem=recv_sem.at[arr, idx],
            device_id={"sp": dev}, device_id_type=MESH)

    def copies(arr):
        return [
            rcopy(arr, 0, own(arr, 0), me, 0, right),
            rcopy(arr, 1, own(arr, 1), me, 1, right),
            rcopy(arr, 2, own(arr, 1), me, 1, left),
            rcopy(arr, 3, own(arr, 0), me, 0, left),
            rcopy(arr, 4, own(arr, 2), me, 2, mate),
            rcopy(arr, 5, piece(arr, left, 0), left, 0, right),
            rcopy(arr, 6, piece(arr, right, 1), right, 1, left),
            rcopy(arr, 7, piece(arr, left, 2), left, 2, mate),
            rcopy(arr, 8, piece(arr, right, 2), right, 2, mate),
            rcopy(arr, 9, piece(arr, opp, 0), opp, 0, mate),
            rcopy(arr, 10, piece(arr, opp, 1), opp, 1, mate),
        ]

    cps = [copies(arr) for arr in range(num)]
    loc = [pltpu.make_async_copy(srcs[arr], piece(arr, me, 2), loc_sem.at[arr]) for arr in range(num)]
    width = SUB * heads // 2
    pairs = heads // 2
    lanes = wt_ref.shape[2]

    @pl.when(step == 0)
    def _():
        barrier = pltpu.get_barrier_semaphore()
        for dev in (left, right, mate):
            pl.semaphore_signal(barrier, inc=1, device_id={"sp": dev}, device_id_type=MESH)
        pl.semaphore_wait(barrier, 3)
        for arr in (2, 0, 1):
            for i in (0, 2, 1, 3, 4):
                cps[arr][i].start()
        for arr in range(num):
            loc[arr].start()
        hp = lax.broadcasted_iota(jnp.int32, (lanes, 2 * width), 0)
        col = lax.broadcasted_iota(jnp.int32, (lanes, 2 * width), 1)
        want_h = me * heads + 2 * lax.rem(col, pairs) + col // width
        want_c = lax.rem(col, width) // pairs
        code = jnp.where(hp == want_h, want_c, -1)
        for c in range(SUB):
            sel[c * lanes:(c + 1) * lanes, :] = jnp.where(code == c, 1.0, 0.0).astype(bf)

    def hand_on(arr):
        cps[arr][0].wait_recv()
        cps[arr][5].start()
        cps[arr][2].wait_recv()
        cps[arr][6].start()

    def to_mate(arr):
        cps[arr][1].wait_recv()
        cps[arr][7].start()
        cps[arr][3].wait_recv()
        cps[arr][8].start()

    @pl.when(step == (5 * last) // 15)
    def _():
        hand_on(2)

    @pl.when(step == (8 * last) // 15)
    def _():
        to_mate(2)

    @pl.when(step == (10 * last) // 15)
    def _():
        hand_on(0)

    @pl.when(step == (12 * last) // 15)
    def _():
        hand_on(1)
        to_mate(0)

    for s in range(CBLK // SUB):
        lhs = jnp.concatenate([wt_ref[s * SUB + i] for i in range(SUB)], axis=1)
        g = dot_nn(lhs, sel[...])
        tn[s] = g[:nope].T
        tr[s] = jnp.concatenate([g[nope:, :width], g[nope:, width:]], axis=0).T
        for h in range(heads):
            par, hp = h % 2, h // 2
            wn_ref[s * SUB:(s + 1) * SUB, h * nope:(h + 1) * nope] = tn[s, pl.ds(par * width + hp, SUB, stride=pairs), :].astype(bf)
        for hp in range(pairs):
            wr_ref[s * SUB:(s + 1) * SUB, hp * LANES:(hp + 1) * LANES] = tr[s, pl.ds(hp, SUB, stride=pairs), :].astype(bf)

    cb = uk_ref.shape[0]
    for i, (src, dst) in enumerate(((uk_ref, uko_ref), (uv_ref, uvo_ref))):
        wd = src.shape[2]
        tu[i] = src[...].astype(jnp.float32).reshape(cb * heads, wd)
        for h in range(heads):
            dst[:, h * wd:(h + 1) * wd] = tu[i, pl.ds(h, cb, stride=heads), :].astype(bf)

    @pl.when(step == last)
    def _():
        to_mate(1)
        for arr in (2, 0, 1):
            cps[arr][5].wait_recv()
            cps[arr][9].start()
            cps[arr][6].wait_recv()
            cps[arr][10].start()
        for arr in range(num):
            for i in (4, 7, 8, 9, 10):
                cps[arr][i].wait_recv()
            for i in range(11):
                cps[arr][i].wait_send()
            loc[arr].wait()


def gather_and_pick(n, heads, nope, kv_own, cs_own, cq_own, w_t, w_uk, w_uv):
    rank = cq_own.shape[1]
    qk = w_t.shape[1]
    kv_rank = w_uk.shape[0]
    vd = w_uv.shape[2]
    steps = rank // CBLK
    cb = kv_rank // steps
    bf = jnp.bfloat16
    f32 = jnp.float32
    const = lambda s: (0, 0)
    own_heads = lambda s: (s, lax.axis_index("sp"), 0)
    return pl.pallas_call(
        functools.partial(gather_kernel, n, heads, nope),
        grid=(steps,),
        in_specs=[
            pl.BlockSpec(kv_own.shape, const),
            pl.BlockSpec(cs_own.shape, const),
            pl.BlockSpec(cq_own.shape, const),
            pl.BlockSpec((CBLK, qk, w_t.shape[2]), lambda s: (s, 0, 0)),
            pl.BlockSpec((cb, heads, nope), own_heads),
            pl.BlockSpec((cb, heads, vd), own_heads),
        ],
        out_specs=[
            pl.BlockSpec(memory_space=pl.ANY),
            pl.BlockSpec(memory_space=pl.ANY),
            pl.BlockSpec(memory_space=pl.ANY),
            pl.BlockSpec((CBLK, heads * nope), lambda s: (s, 0)),
            pl.BlockSpec((CBLK, heads * (qk - nope)), lambda s: (s, 0)),
            pl.BlockSpec((cb, heads * nope), lambda s: (s, 0)),
            pl.BlockSpec((cb, heads * vd), lambda s: (s, 0)),
        ],
        out_shape=[
            jax.ShapeDtypeStruct((n * kv_own.shape[0], kv_own.shape[1]), bf),
            jax.ShapeDtypeStruct((n * cs_own.shape[0], cs_own.shape[1]), f32),
            jax.ShapeDtypeStruct((n * cq_own.shape[0], rank), bf),
            jax.ShapeDtypeStruct((rank, heads * nope), bf),
            jax.ShapeDtypeStruct((rank, heads * (qk - nope)), bf),
            jax.ShapeDtypeStruct((kv_rank, heads * nope), bf),
            jax.ShapeDtypeStruct((kv_rank, heads * vd), bf),
        ],
        scratch_shapes=[
            pltpu.VMEM((SUB * w_t.shape[2], SUB * heads), bf),
            pltpu.VMEM((CBLK // SUB, SUB * heads, nope), f32),
            pltpu.VMEM((CBLK // SUB, SUB * heads // 2, LANES), f32),
            pltpu.VMEM((2, cb * heads, nope), f32),
            pltpu.SemaphoreType.DMA((3, 11)),
            pltpu.SemaphoreType.DMA((3, 11)),
            pltpu.SemaphoreType.DMA((3,)),
        ],
        compiler_params=pltpu.CompilerParams(collective_id=0, has_side_effects=True, dimension_semantics=("arbitrary",), vmem_limit_bytes=60_000_000),
        cost_estimate=pl.CostEstimate(flops=30_000_000_000, bytes_accessed=90_000_000, transcendentals=0),
        name="gather_pick",
    )(kv_own, cs_own, cq_own, w_t, w_uk, w_uv)


QB = 512
CH = 16


def attn_kernel(g, scale2, kv_rank, nope, rot, kv_ref, cq_ref, cs_ref, wn_hbm, wr_hbm, uk_ref, uv_ref, o_ref, wn_ref, wr_ref, wsem, kcat, vt, uvt, qcat, acc, mrow, lrow, s0, s1, p0, p1, mx0, mx1, al0, al1):
    b = pl.program_id(0)
    vd = uv_ref.shape[1] // GROUP
    bf = jnp.bfloat16
    sbuf, pbuf, mxb, alb = (s0, s1), (p0, p1), (mx0, mx1), (al0, al1)
    hd = rot // 2
    hb = QB // 2

    @pl.when(b == 0)
    def _():
        loads = [
            pltpu.make_async_copy(src.at[:, pl.ds(g * dst.shape[1], dst.shape[1])], dst, wsem.at[i])
            for i, (src, dst) in enumerate(((wn_hbm, wn_ref), (wr_hbm, wr_ref)))
        ]
        for c in loads:
            c.start()
        uvt[...] = uv_ref[...].T

        def fill(i, _):
            r = pl.ds(pl.multiple_of(i * QB, QB), QB)
            c = kv_ref[r, :kv_rank]
            k = dot_nn(c, uk_ref[...]).astype(bf)
            pe_f = kv_ref[r, kv_rank:kv_rank + LANES].astype(jnp.float32)
            pe = (pe_f.astype(bf), pltpu.roll(pe_f, rot, 1).astype(bf))
            for h in range(GROUP):
                kcat[h, r, :nope] = k[:, h * nope:(h + 1) * nope]
                kcat[h, r, nope:] = pe[h % 2]
            vt[:, r] = dot_nt(uvt[...], c).astype(bf)
            return 0
        lax.fori_loop(0, kv_ref.shape[0] // QB, fill, 0)
        for c in loads:
            c.wait()

    cq = cq_ref[...]
    qn = dot_nn(cq, wn_ref[...]).astype(bf)
    qr = dot_nn(cq, wr_ref[...])
    per = cs_ref.shape[1]
    cos_p, sin_p = [], []
    for j in range(QB // per):
        c_t = cs_ref[j * rot:j * rot + hd, :]
        s_t = cs_ref[j * rot + hd:(j + 1) * rot, :]
        cos_p.append(jnp.concatenate([c_t] * (LANES // hd), axis=0).T)
        sin_p.append(jnp.concatenate([-s_t, s_t] * (LANES // rot), axis=0).T)
    cos_t = jnp.concatenate(cos_p, axis=0)
    sin_t = jnp.concatenate(sin_p, axis=0)
    for pr in range(GROUP // 2):
        z = qr[:, pr * LANES:(pr + 1) * LANES]
        lane = lax.broadcasted_iota(jnp.int32, z.shape, 1)
        swapped = jnp.where((lane // hd) % 2 == 0, pltpu.roll(z, LANES - hd, 1), pltpu.roll(z, hd, 1))
        zr = (z * cos_t + swapped * sin_t).astype(bf)
        for m in range(2):
            h = 2 * pr + m
            qcat[h, :, :nope] = qn[:, h * nope:(h + 1) * nope]
            qcat[h, :, nope:] = zr

    r0 = pl.multiple_of(b * QB, QB)
    tri = lax.broadcasted_iota(jnp.int32, (hb, hb), 0) <= lax.broadcasted_iota(jnp.int32, (hb, hb), 1)

    def score(h, r, slot):
        m = None
        for c in (0, hb):
            s = dot_nt(kcat[h, pl.ds(r + c, hb), :], qcat[h])
            sbuf[slot][c:c + hb, :] = s
            mc = jnp.max(s, axis=0, keepdims=True)
            m = mc if m is None else jnp.maximum(m, mc)
        mxb[slot][...] = m

    def soft(h, slot):
        m_old = mrow[h]
        m_new = jnp.maximum(m_old, mxb[slot][...])
        alpha = jnp.exp2((m_old - m_new) * scale2)
        tot = None
        for c in range(0, QB, CH):
            p = jnp.exp2((sbuf[slot][c:c + CH, :] - m_new) * scale2)
            pbuf[slot][c:c + CH, :] = p.astype(bf)
            part = jnp.sum(p.reshape(CH // 8, 8, QB), axis=0)
            tot = part if tot is None else tot + part
        lrow[h] = lrow[h] * alpha + jnp.sum(tot, axis=0, keepdims=True)
        mrow[h] = m_new
        alb[slot][...] = alpha

    def weigh(h, r, slot):
        v = vt[h * vd:(h + 1) * vd, pl.ds(r, QB)]
        acc[h] = acc[h] * alb[slot][...] + dot_nn(v, pbuf[slot][...])

    def score_diag(h, slot):
        k = kcat[h, pl.ds(r0, QB), :]
        q = qcat[h]
        sa = dot_nt(k[:hb], q)
        sa0 = jnp.where(tri, sa[:, :hb], NEG)
        sa1 = sa[:, hb:]
        sb = jnp.where(tri, dot_nt(k[hb:], q[hb:]), NEG)
        sbuf[slot][:hb, :hb] = sa0
        sbuf[slot][:hb, hb:] = sa1
        sbuf[slot][hb:, hb:] = sb
        mxb[slot][:, :hb] = jnp.max(sa0, axis=0, keepdims=True)
        mxb[slot][:, hb:] = jnp.maximum(jnp.max(sa1, axis=0, keepdims=True), jnp.max(sb, axis=0, keepdims=True))

    def soft_diag(h, slot):
        m = mxb[slot][...]
        ta = tb = None
        for c in range(0, hb, CH):
            pa = jnp.exp2((sbuf[slot][c:c + CH, :] - m) * scale2)
            pbuf[slot][c:c + CH, :] = pa.astype(bf)
            part = jnp.sum(pa.reshape(CH // 8, 8, QB), axis=0)
            ta = part if ta is None else ta + part
        for c in range(hb, QB, CH):
            pb = jnp.exp2((sbuf[slot][c:c + CH, hb:] - m[:, hb:]) * scale2)
            pbuf[slot][c:c + CH, hb:] = pb.astype(bf)
            part = jnp.sum(pb.reshape(CH // 8, 8, hb), axis=0)
            tb = part if tb is None else tb + part
        lrow[h, :, :hb] = jnp.sum(ta[:, :hb], axis=0, keepdims=True)
        lrow[h, :, hb:] = jnp.sum(ta[:, hb:] + tb, axis=0, keepdims=True)
        mrow[h] = m

    def weigh_diag(h, slot):
        rows = slice(h * vd, (h + 1) * vd)
        acc[h, :, :hb] = dot_nn(vt[rows, pl.ds(r0, hb)], pbuf[slot][:hb, :hb])
        acc[h, :, hb:] = dot_nn(vt[rows, pl.ds(r0, QB)], pbuf[slot][:, hb:])

    score_diag(0, 0)
    for h in range(GROUP):
        if h + 1 < GROUP:
            score_diag(h + 1, (h + 1) % 2)
        else:
            score(0, 0, 0)
        soft_diag(h, h % 2)
        weigh_diag(h, h % 2)

    def body(kb, _):
        r = pl.multiple_of(kb * QB, QB)
        for h in range(GROUP):
            if h + 1 < GROUP:
                score(h + 1, r, (h + 1) % 2)
            else:
                score(0, pl.multiple_of(r + QB, QB), 0)
            soft(h, h % 2)
            weigh(h, r, h % 2)
        return 0

    lax.fori_loop(0, b, body, 0)

    for h in range(GROUP):
        o_ref[:, h * vd:(h + 1) * vd] = (acc[h] * (1.0 / lrow[h])).T.astype(bf)


def attention_group(g, scale2, kv_rank, nope, rot, vd, kv_all, cq_all, cs_all, wn, wr, uk, uv):
    seq, rank = cq_all.shape
    bf = jnp.bfloat16
    f32 = jnp.float32
    pairs = seq * (seq + QB) // 2
    blocks = seq // QB
    flops = 2 * GROUP * (seq * rank * (nope + rot) + seq * kv_rank * (nope + vd) + pairs * (nope + rot + vd) * 2)
    row = pltpu.VMEM((1, QB), f32)
    return pl.pallas_call(
        functools.partial(attn_kernel, g, scale2, kv_rank, nope, rot),
        grid=(blocks,),
        in_specs=[
            pl.BlockSpec(kv_all.shape, lambda b: (0, 0)),
            pl.BlockSpec((QB, rank), lambda b: (b, 0)),
            pl.BlockSpec((cs_all.shape[0] // blocks, cs_all.shape[1]), lambda b: (b, 0)),
            pl.BlockSpec(memory_space=pl.ANY),
            pl.BlockSpec(memory_space=pl.ANY),
            pl.BlockSpec((kv_rank, GROUP * nope), lambda b: (0, g)),
            pl.BlockSpec((kv_rank, GROUP * vd), lambda b: (0, g)),
        ],
        out_specs=pl.BlockSpec((QB, GROUP * vd), lambda b: (b, 0)),
        out_shape=jax.ShapeDtypeStruct((seq, GROUP * vd), bf),
        scratch_shapes=[
            pltpu.VMEM((rank, GROUP * nope), bf),
            pltpu.VMEM((rank, GROUP * rot), bf),
            pltpu.SemaphoreType.DMA((2,)),
            pltpu.VMEM((GROUP, seq, nope + LANES), bf),
            pltpu.VMEM((GROUP * vd, seq), bf),
            pltpu.VMEM((GROUP * vd, kv_rank), bf),
            pltpu.VMEM((GROUP, QB, nope + LANES), bf),
            pltpu.VMEM((GROUP, vd, QB), f32),
            pltpu.VMEM((GROUP, 1, QB), f32),
            pltpu.VMEM((GROUP, 1, QB), f32),
            pltpu.VMEM((QB, QB), f32),
            pltpu.VMEM((QB, QB), f32),
            pltpu.VMEM((QB, QB), bf),
            pltpu.VMEM((QB, QB), bf),
            row, row, row, row,
        ],
        compiler_params=pltpu.CompilerParams(dimension_semantics=("arbitrary",), vmem_limit_bytes=60_000_000),
        cost_estimate=pl.CostEstimate(flops=flops, bytes_accessed=12_000_000, transcendentals=pairs * GROUP),
        name="mla_attn",
    )(kv_all, cq_all, cs_all, wn, wr, uk, uv)


OSLOTS = 6
NT = 512
NH = 4


def out_kernel(n, call, first, *refs):
    if first:
        o_ref, w_ref, out_ref, wbuf, acc, sem, acc_sem = refs
    else:
        acc_in, o_ref, w_ref, out_ref, wbuf, acc, prev, sem, acc_sem = refs
    rows = o_ref.shape[0] // n
    hidden = w_ref.shape[3]
    wide = hidden // NH
    steps = NH * n

    def copy(s, slot):
        cols = pl.ds(pl.multiple_of(lax.rem(s, NH) * wide, LANES), wide)
        return pltpu.make_async_copy(w_ref.at[s // NH, call, :, cols], wbuf.at[slot], sem.at[slot])

    for s in range(OSLOTS - 1):
        copy(s, s).start()
    if not first:
        pltpu.make_async_copy(acc_in, prev, acc_sem).start()
    acc[...] = jnp.zeros_like(acc)

    def body(s, _):
        slot = lax.rem(s, OSLOTS)

        @pl.when(s + OSLOTS - 1 < steps)
        def _():
            copy(s + OSLOTS - 1, lax.rem(s + OSLOTS - 1, OSLOTS)).start()
        copy(s, slot).wait()
        lhs = o_ref[pl.ds(pl.multiple_of((s // NH) * rows, rows), rows), :]
        side = lax.rem(s, NH)
        for t in range(0, wide, NT):
            cols = slice(t, min(t + NT, wide))
            acc[side, :, cols] += dot_nn(lhs, wbuf[slot, :, cols])
        return 0

    lax.fori_loop(0, steps, body, 0)
    if first:
        pltpu.make_async_copy(acc, out_ref, acc_sem).start()
        pltpu.make_async_copy(acc, out_ref, acc_sem).wait()
    else:
        pltpu.make_async_copy(acc_in, prev, acc_sem).wait()
        for i in range(NH):
            out_ref[:, i * wide:(i + 1) * wide] = (prev[i] + acc[i]).astype(out_ref.dtype)


def out_product(acc, o, w4, call, n):
    seq, width = o.shape
    rows = seq // n
    hidden = w4.shape[3]
    first = acc is None
    anyspec = pl.BlockSpec(memory_space=pl.ANY)
    vm = pl.BlockSpec(memory_space=pltpu.VMEM)
    args = ([] if first else [acc]) + [o, w4]
    sums = pltpu.VMEM((NH, rows, hidden // NH), jnp.float32)
    return pl.pallas_call(
        functools.partial(out_kernel, n, call, first),
        in_specs=([] if first else [anyspec]) + [vm, anyspec],
        out_specs=anyspec if first else vm,
        out_shape=jax.ShapeDtypeStruct((NH, rows, hidden // NH), jnp.float32) if first else jax.ShapeDtypeStruct((rows, hidden), jnp.bfloat16),
        scratch_shapes=[
            pltpu.VMEM((OSLOTS, width, hidden // NH), jnp.bfloat16),
            sums,
        ] + ([] if first else [sums]) + [
            pltpu.SemaphoreType.DMA((OSLOTS,)),
            pltpu.SemaphoreType.DMA,
        ],
        compiler_params=pltpu.CompilerParams(vmem_limit_bytes=60_000_000),
        cost_estimate=pl.CostEstimate(flops=2 * rows * hidden * width * n, bytes_accessed=2 * hidden * width * n, transcendentals=0),
        name="out_product",
    )(*args)


def solution(mesh):
    n = mesh.shape['sp']
    rows_spec = P(('dp', 'sp'), None)
    tok_spec = P(('dp', 'sp'))
    rep = P()

    def local_step(tok_in, tok_pos, w_dq, g_q, w_uq, w_dkv, g_kv, w_uk, w_uv, w_o):
        num_heads = w_uq.shape[1]
        heads = num_heads // n
        qk_dim = w_uq.shape[2]
        kv_rank = g_kv.shape[0]
        rot = w_dkv.shape[1] - kv_rank
        nope = qk_dim - rot
        vd = w_uv.shape[2]
        scale2 = (0.1 * math.log(YARN_FACTOR) + 1.0) ** 2 / math.sqrt(qk_dim) / math.log(2.0)

        angles = rope_freqs(rot)[:, None] * tok_pos.astype(jnp.float32)[None, :]
        cs_own = jnp.concatenate([jnp.cos(angles), jnp.sin(angles)], axis=0)
        cq_own, cache_kv, cache_pe, kv_own = latents(tok_in, w_dq, w_dkv, g_q, g_kv, cs_own)

        w_t = jnp.transpose(w_uq, (0, 2, 1))
        kv_all, cs_all, cq_all, wn, wr, uk, uv = gather_and_pick(n, heads, nope, kv_own, cs_own, cq_own, w_t, w_uk, w_uv)

        chunks = heads // GROUP
        o_parts = []
        for g in range(chunks):
            o_g = attention_group(g, scale2, kv_rank, nope, rot, vd, kv_all, cq_all, cs_all, wn, wr, uk, uv)
            o_parts.append(lax.all_to_all(o_g, 'sp', 0, 0, tiled=True))
        w4 = w_o.reshape(n, chunks, GROUP * vd, w_o.shape[2])
        acc = None
        for call in range(chunks):
            acc = out_product(acc, o_parts[call], w4, call, n)
        return acc, cache_kv, cache_pe

    return jax.shard_map(local_step, mesh=mesh, in_specs=(rows_spec, tok_spec, rep, rep, rep, rep, rep, rep, rep, rep), out_specs=(rows_spec, rows_spec, rows_spec), check_vma=False)
```
